32 devices in a mesh: rep: 8 (over z, x), fsdp: 2 (over y), seq: 2 (over core).
Axes of the slice: x: 2, y: 2, z: 4, core: 2. Of those that a mesh axis runs over, the one named last changes fastest.
Arguments:
- tokens: bfloat16 [32768, 1024], P(('rep', 'fsdp', 'seq')), may hold values from -6 to 6
- segments: int32 [16, 2048], P(('rep', 'fsdp')), may hold values from 0 to 15, never falling along the last dimension, each value on 1 to 1024 neighbouring positions
- attn_norm: bfloat16 [1024], P(('fsdp', 'seq')), may hold values from 0.5 to 1.5
- w_q: bfloat16 [1024, 2048], P(('fsdp', 'seq')), may hold values from -0.1875 to 0.1875
- w_k: bfloat16 [1024, 1024], P(('fsdp', 'seq')), may hold values from -0.1875 to 0.1875
- w_v: bfloat16 [1024, 1024], P(('fsdp', 'seq')), may hold values from -0.1875 to 0.1875
- q_norm: bfloat16 [128], P(('fsdp', 'seq')), may hold values from 0.5 to 1.5
- k_norm: bfloat16 [128], P(('fsdp', 'seq')), may hold values from 0.5 to 1.5
- w_o: bfloat16 [2048, 1024], P(('fsdp', 'seq')), may hold values from -1 to 1
- mlp_norm: bfloat16 [1024], P(('fsdp', 'seq')), may hold values from 0.5 to 1.5
- w_gate: bfloat16 [1024, 3072], P(('fsdp', 'seq')), may hold values from -0.1875 to 0.1875
- w_up: bfloat16 [1024, 3072], P(('fsdp', 'seq')), may hold values from -0.1875 to 0.1875
- w_down: bfloat16 [3072, 1024], P(('fsdp', 'seq')), may hold values from -0.109375 to 0.109375
- cotangent: bfloat16 [32768, 1024], P(('rep', 'fsdp', 'seq')), may hold values from -6 to 6
Outputs:
- output: bfloat16 [32768, 1024], P(('rep', 'fsdp', 'seq'))
- tokens_grad: float32 [32768, 1024], P(('rep', 'fsdp', 'seq'))
- grad_attn_norm: float32 [1024], P(('fsdp', 'seq'))
- grad_w_q: float32 [1024, 2048], P(('fsdp', 'seq'))
- grad_w_k: float32 [1024, 1024], P(('fsdp', 'seq'))
- grad_w_v: float32 [1024, 1024], P(('fsdp', 'seq'))
- grad_q_norm: float32 [128], P(('fsdp', 'seq'))
- grad_k_norm: float32 [128], P(('fsdp', 'seq'))
- grad_w_o: float32 [2048, 1024], P(('fsdp', 'seq'))
- grad_mlp_norm: float32 [1024], P(('fsdp', 'seq'))
- grad_w_gate: float32 [1024, 3072], P(('fsdp', 'seq'))
- grad_w_up: float32 [1024, 3072], P(('fsdp', 'seq'))
- grad_w_down: float32 [3072, 1024], P(('fsdp', 'seq'))
The draws below stay inside these ranges and needn't reach their ends.
Inputs may be any that keep to these rules, and one draw needn't show every extreme that they name: `segments`: within each sequence the segment numbers never fall, every number from 0 to the largest appears, each document has 1 to 1024 tokens and one has exactly 1024.
All inputs are finite; a program needn't handle non-finite values.
Results may differ from the reference program's by a relative error of at most 0.013.
Values may be sent and summed in bfloat16 or wider, within the bound.
No kernel may reach another device: no remote copies, remote signals or barrier semaphores. Data moves between devices by JAX's collectives and lax.ppermute only.
A program may use at most 512 MiB of HBM per device.

```python
import math
import jax
import jax.numpy as jnp
import numpy as np
from jax import lax

D = 1024
HQ = 16
KV = 8
HD = 128
FF = 3072
LEN = 2048
SEQS = 16
TOKENS = 32768


def shard_levels(key, dims, cuts, low, largest):
    def one(dim, blocks):
        heights = jax.random.uniform(jax.random.fold_in(jax.random.fold_in(key, 6), dim), (blocks,), jnp.float32, low / len(cuts), largest / len(cuts))
        return jnp.repeat(jnp.exp(heights), dims[dim] // blocks).reshape((-1,) + (1,) * (len(dims) - dim - 1))

    level = one(*cuts[0])
    for cut in cuts[1:]:
        level = level * one(*cut)
    return level


def split_up(number_of, total, most, lean):
    loads = [(1 << 20) // math.isqrt(rank ** lean) + 1 for rank in range(2, number_of + 1)]
    spare, counts = total - most - (number_of - 1), [1] * (number_of - 1)
    while spare > 0:
        candidates = [i for i in range(number_of - 1) if counts[i] < most]
        pool, left = sum([loads[i] for i in candidates]), spare
        for i in candidates:
            extra = min(most - counts[i], max(1, left * loads[i] // pool), spare)
            counts[i] = counts[i] + extra
            spare = spare - extra
    return np.array([most] + counts)


def ragged_sizes(rng, number_of, total, bound, lean):
    if number_of == 2:
        one = jax.random.randint(rng, (), max(1, total - bound), min(bound, total - 1) + 1)
        return jnp.stack([one, total - one])
    tallies = jnp.asarray(split_up(number_of, total, bound, lean), jnp.int32)
    couples = (number_of - 1) // 2
    source_of, receiver = tallies[1:1 + 2 * couples:2], tallies[2:2 + 2 * couples:2]
    slack = jnp.minimum(source_of - 1, bound - receiver)
    moved = jax.random.randint(jax.random.fold_in(rng, 1), (couples,), 0, 1 << 20) % (slack + 1)
    tallies = tallies.at[1:1 + 2 * couples:2].set(source_of - moved).at[2:2 + 2 * couples:2].set(receiver + moved)
    return tallies[jax.random.permutation(jax.random.fold_in(rng, 2), number_of)]


def noise(stream_key, shape, scale, reach, cuts=(), held_as=jnp.bfloat16):
    entries = jax.random.normal(stream_key, shape, jnp.float32) * scale
    if len(cuts) > 0:
        entries = shard_levels(stream_key, shape, cuts, -0.22, 0.18) * entries
    return jnp.clip(entries, min=-reach, max=reach).astype(held_as)


def setup_inputs(seed: int = 0) -> dict:
    splits = jax.random.split(jax.random.key(seed), 15)
    tokens = noise(splits[0], (TOKENS, D), 1.0, 6.0, ((0, 32),))
    segments = jax.vmap(lambda own: jnp.searchsorted(jnp.cumsum(ragged_sizes(own, max(4, LEN // 128), LEN, LEN // 2, 2)), jnp.arange(LEN), side="right"))(jax.random.split(splits[1], SEQS)).reshape((SEQS, LEN)).astype(jnp.int32)
    attn_norm = jnp.clip(1.0 + 0.1 * jax.random.normal(splits[2], (D,), jnp.float32), 0.5, 1.5).astype(jnp.bfloat16)
    w_q = noise(splits[3], (D, HQ * HD), D ** -0.5, 0.1875, ((0, 4),))
    w_k = noise(splits[4], (D, KV * HD), D ** -0.5, 0.1875, ((0, 4),))
    w_v = noise(splits[5], (D, KV * HD), D ** -0.5, 0.1875, ((0, 4),))
    q_norm = jnp.clip(1.0 + 0.1 * jax.random.normal(splits[6], (HD,), jnp.float32), 0.5, 1.5).astype(jnp.bfloat16)
    k_norm = jnp.clip(1.0 + 0.1 * jax.random.normal(splits[7], (HD,), jnp.float32), 0.5, 1.5).astype(jnp.bfloat16)
    w_o = noise(splits[8], (HQ * HD, D), (max(HQ * HD // 64, 1)) ** -0.5, 1.0, ((0, 4),))
    mlp_norm = jnp.clip(1.0 + 0.1 * jax.random.normal(splits[9], (D,), jnp.float32), 0.5, 1.5).astype(jnp.bfloat16)
    w_gate = noise(splits[10], (D, FF), D ** -0.5, 0.1875, ((0, 4),))
    w_up = noise(splits[11], (D, FF), D ** -0.5, 0.1875, ((0, 4),))
    w_down = noise(splits[12], (FF, D), FF ** -0.5, 0.109375, ((0, 4),))
    cotangent = noise(splits[13], (TOKENS, D), 1.0, 6.0, ((0, 32),))
    return {"tokens": tokens, "segments": segments, "attn_norm": attn_norm, "w_q": w_q, "w_k": w_k, "w_v": w_v, "q_norm": q_norm, "k_norm": k_norm, "w_o": w_o, "mlp_norm": mlp_norm, "w_gate": w_gate, "w_up": w_up, "w_down": w_down, "cotangent": cotangent}


EPSILON = 1e-06
ROPE_BASE = 1000000.0
MASKED = -1e+30
FULL_PRECISION = lax.Precision.HIGHEST

@jax.custom_vjp
def low(v):
    return lax.optimization_barrier(v.astype(jnp.bfloat16)).astype(jnp.float32)

@jax.custom_vjp
def low_back(v):
    return v

def low_keep(v):
    return (low(v), None)

def low_pass(kept, grad):
    return (grad,)

def back_keep(v):
    return (v, None)

def back_low(kept, grad):
    return (low(grad),)
low.defvjp(low_keep, low_pass)
low_back.defvjp(back_keep, back_low)

def rms_scale(values, gain_vec):
    return values * lax.rsqrt(lax.optimization_barrier(jnp.mean(values * values, axis=-1, keepdims=True)) + EPSILON) * gain_vec

def rotate(values, cosine, sine_tab):
    half_width = values.shape[-1] // 2
    turned = jnp.concatenate([-values[..., half_width:], values[..., :half_width]], axis=-1)
    return values * cosine + turned * sine_tab

def rope_tables(seg_row):
    length = seg_row.shape[0]
    before = lax.optimization_barrier(jnp.sum((seg_row[None, :] < seg_row[:, None]).astype(jnp.int32), axis=1))
    position = (jnp.arange(length, dtype=jnp.int32) - before).astype(jnp.float32)
    freq_index = jnp.arange(HD // 2, dtype=jnp.float32)
    inverse = ROPE_BASE ** (freq_index * (-2.0 / HD))
    angles = position[:, None] * inverse[None, :]
    angles = jnp.concatenate([angles, angles], axis=1)
    return (jnp.cos(angles), jnp.sin(angles))

def layer_forward(hidden_in, attn_gain, w_q, w_k, w_v, q_gain, k_gain, w_o, mlp_gain, w_gate, w_up, w_down, seg_row, cosine, sine_tab):
    length = hidden_in.shape[0]
    groups = HQ // KV
    scaling = HD ** (-0.5)
    normed = low(rms_scale(hidden_in, attn_gain))
    query_raw = low_back(jnp.dot(normed, w_q, precision=FULL_PRECISION)).reshape(length, HQ, HD)
    key_raw = low_back(jnp.dot(normed, w_k, precision=FULL_PRECISION)).reshape(length, KV, HD)
    value_rows = low(low_back(jnp.dot(normed, w_v, precision=FULL_PRECISION))).reshape(length, KV, HD)
    queries = low(rotate(rms_scale(query_raw, q_gain), cosine[:, None, :], sine_tab[:, None, :]))
    key_rows = low(rotate(rms_scale(key_raw, k_gain), cosine[:, None, :], sine_tab[:, None, :]))
    queries = queries.reshape(length, KV, groups, HD)
    positions = jnp.arange(length, dtype=jnp.int32)
    block_rows = min(512, length)

    def one_block(start_row):
        query_block = lax.dynamic_slice_in_dim(queries, start_row, block_rows, 0)
        row_index = start_row + jnp.arange(block_rows, dtype=jnp.int32)
        row_seg = lax.dynamic_slice_in_dim(seg_row, start_row, block_rows, 0)
        allowed = (positions[None, :] <= row_index[:, None]) & (seg_row[None, :] == row_seg[:, None])
        raw_scores = low_back(jnp.einsum('qkgd,skd->kgqs', query_block, key_rows, precision=FULL_PRECISION))
        scores = jnp.where(allowed[None, None], raw_scores * scaling, MASKED)
        highest = lax.optimization_barrier(jnp.max(scores, axis=-1, keepdims=True))
        weights = jnp.exp(scores - highest)
        probs = low(weights / lax.optimization_barrier(jnp.sum(weights, axis=-1, keepdims=True)))
        mixed = jnp.einsum('kgqs,skd->qkgd', probs, value_rows, precision=FULL_PRECISION)
        return mixed.reshape(block_rows, HQ * HD)
    starts = jnp.arange(length // block_rows, dtype=jnp.int32) * block_rows
    mixed = lax.map(jax.checkpoint(one_block), starts).reshape(length, HQ * HD)
    attended = low(low_back(mixed))
    middle = hidden_in + low_back(jnp.dot(attended, w_o, precision=FULL_PRECISION))
    mlp_in = low(rms_scale(middle, mlp_gain))
    gate_val = low_back(jnp.dot(mlp_in, w_gate, precision=FULL_PRECISION))
    up_val = low_back(jnp.dot(mlp_in, w_up, precision=FULL_PRECISION))
    hidden_act = low(gate_val / (1.0 + jnp.exp(-gate_val)) * up_val)
    return middle + low_back(jnp.dot(hidden_act, w_down, precision=FULL_PRECISION))

def reference(tokens, segments, attn_norm, w_q, w_k, w_v, q_norm, k_norm, w_o, mlp_norm, w_gate, w_up, w_down, cotangent):
    params = tuple((member.astype(jnp.float32) for member in (attn_norm, w_q, w_k, w_v, q_norm, k_norm, w_o, mlp_norm, w_gate, w_up, w_down)))
    inputs = tokens.astype(jnp.float32).reshape(SEQS, LEN, D)
    grads_in = cotangent.astype(jnp.float32).reshape(SEQS, LEN, D)

    def one_sequence(totals, member):
        hidden_in, grad_out, seg_row = member
        cosine, sine_tab = rope_tables(seg_row)

        def apply_layer(hidden_val, *weights):
            return layer_forward(hidden_val, *weights, seg_row, cosine, sine_tab)
        result, pullback = jax.vjp(apply_layer, hidden_in, *params)
        gradients = pullback(grad_out)
        totals = tuple((summed + partial_grad for summed, partial_grad in zip(totals, gradients[1:])))
        return (totals, (result.astype(jnp.bfloat16), gradients[0]))
    zeros_init = tuple((jnp.zeros_like(member) for member in params))
    totals, (results, input_grads) = lax.scan(one_sequence, zeros_init, (inputs, grads_in, segments))
    return (results.reshape(TOKENS, D), input_grads.reshape(TOKENS, D), totals[0], totals[1], totals[2], totals[3], totals[4], totals[5], totals[6], totals[7], totals[8], totals[9], totals[10])
```

```python
import jax
import jax.numpy as jnp
from jax import lax
from jax.experimental import pallas as pl
from jax.experimental.pallas import tpu as pltpu
from jax.sharding import PartitionSpec as P

HQ = 16
KV = 8
HD = 128
EPSILON = 1e-06
ROPE_BASE = 1000000.0
SCALE = HD**-0.5
LOG2E = 1.4426950408889634
BLK = 256
BF = jnp.bfloat16
F32 = jnp.float32


def nn(a, b):
    return lax.dot_general(a, b, (((1,), (0,)), ((), ())), preferred_element_type=F32)


def nt(a, b):
    return lax.dot_general(a, b, (((1,), (1,)), ((), ())), preferred_element_type=F32)


def tn(a, b):
    return lax.dot_general(a, b, (((0,), (0,)), ((), ())), preferred_element_type=F32)


def full_spec(shape):
    return pl.BlockSpec(shape, lambda *_: (0,) * len(shape), pipeline_mode=pl.Buffered(1))


def qkv_kernel(x_ref, gain_ref, w_ref, cos_ref, sin_ref, hg_ref, normed_ref, qkv_ref, raw_ref):
    x = x_ref[...].astype(F32)
    scale = lax.rsqrt(jnp.mean(x * x, axis=1, keepdims=True) + EPSILON)
    normed = (x * scale * gain_ref[...]).astype(BF)
    normed_ref[...] = normed
    cosine = cos_ref[...]
    sine = sin_ref[...]
    groups = w_ref.shape[1] // (4 * HD)
    for g in range(groups):
        acc = nn(normed, w_ref[:, g * 512 : (g + 1) * 512])
        for h in range(3):
            t = acc[:, h * HD : (h + 1) * HD]
            gain = hg_ref[0:1, :] if h < 2 else hg_ref[1:2, :]
            n = t * lax.rsqrt(jnp.mean(t * t, axis=1, keepdims=True) + EPSILON) * gain
            turned = n * cosine + pltpu.roll(n, HD // 2, 1) * sine
            qkv_ref[:, g * 512 + h * HD : g * 512 + (h + 1) * HD] = turned.astype(BF)
            raw_ref[:, g * 384 + h * HD : g * 384 + (h + 1) * HD] = t.astype(BF)
        qkv_ref[:, g * 512 + 384 : (g + 1) * 512] = acc[:, 384:].astype(BF)


def project(x_all, gain, w_qkv, cosine, sine, head_gains):
    length, width = x_all.shape
    cols = w_qkv.shape[1]
    rows = lambda n: pl.BlockSpec((BLK, n), lambda t: (t, 0))
    return pl.pallas_call(
        qkv_kernel,
        grid=(length // BLK,),
        in_specs=[
            rows(width),
            full_spec((1, width)),
            full_spec((width, cols)),
            rows(HD),
            rows(HD),
            full_spec((2, HD)),
        ],
        out_specs=[rows(width), rows(cols), rows(cols // 4 * 3)],
        out_shape=[
            jax.ShapeDtypeStruct((length, width), BF),
            jax.ShapeDtypeStruct((length, cols), BF),
            jax.ShapeDtypeStruct((length, cols // 4 * 3), BF),
        ],
        name="project",
    )(x_all, gain, w_qkv, cosine, sine, head_gains)


def stack_heads(block):
    return jnp.concatenate([block[:, :HD], block[:, HD:]], axis=0)


def attend_kernel(low_ref, qkv_ref, start_ref, out_ref, lse_ref, acc, total):
    blocks = qkv_ref.shape[0] // BLK

    def query_block(qb, carry):
        r0 = pl.multiple_of(qb * BLK, BLK)
        q2 = stack_heads(qkv_ref[pl.ds(r0, BLK), 0:256])
        first = start_ref[pl.ds(r0, BLK), :]
        first2 = jnp.concatenate([first, first], axis=0)

        def tile(k0, diagonal):
            k = qkv_ref[pl.ds(k0, BLK), 256:384]
            v = qkv_ref[pl.ds(k0, BLK), 384:512]
            s = nt(q2, k) * (SCALE * LOG2E)
            col = lax.broadcasted_iota(jnp.int32, (2 * BLK, BLK), 1)
            mask = col >= first2 - k0
            if diagonal:
                row = lax.broadcasted_iota(jnp.int32, (2 * BLK, BLK), 0) & (BLK - 1)
                mask = mask & (col <= row)
            p = jnp.where(mask, jnp.exp2(s), 0.0)
            part = p[:, :HD]
            for n in range(1, BLK // HD):
                part = part + p[:, n * HD : (n + 1) * HD]
            return part, nn(p.astype(BF), v)

        part, mixed = tile(r0, True)
        total[...] = part
        acc[...] = mixed

        def step(kb, inner):
            more, mixed_more = tile(pl.multiple_of(kb * BLK, BLK), False)
            total[...] += more
            acc[...] += mixed_more
            return inner

        lax.fori_loop(low_ref[qb], qb, step, 0)
        sums = total[...]
        o = (acc[...] / jnp.sum(sums, axis=1, keepdims=True)).astype(BF)
        out_ref[pl.ds(r0, BLK), 0:HD] = o[:BLK]
        out_ref[pl.ds(r0, BLK), HD : 2 * HD] = o[BLK:]
        line = jnp.log2(jnp.sum(jnp.transpose(sums), axis=0, keepdims=True))
        lse_ref[0, 0:1, pl.ds(r0, BLK)] = line[:, :BLK]
        lse_ref[0, 1:2, pl.ds(r0, BLK)] = line[:, BLK:]
        return carry

    lax.fori_loop(0, blocks, query_block, 0)


def attend(low, qkv, start):
    length, cols = qkv.shape
    groups = cols // 512
    return pl.pallas_call(
        attend_kernel,
        grid_spec=pltpu.PrefetchScalarGridSpec(
            num_scalar_prefetch=1,
            grid=(groups,),
            in_specs=[
                pl.BlockSpec((length, 512), lambda g, low: (0, g)),
                full_spec((length, 1)),
            ],
            out_specs=[
                pl.BlockSpec((length, 256), lambda g, low: (0, g)),
                pl.BlockSpec((1, 2, length), lambda g, low: (g, 0, 0)),
            ],
            scratch_shapes=[
                pltpu.VMEM((2 * BLK, HD), F32),
                pltpu.VMEM((2 * BLK, HD), F32),
            ],
        ),
        out_shape=[
            jax.ShapeDtypeStruct((length, groups * 256), BF),
            jax.ShapeDtypeStruct((groups, 2, length), F32),
        ],
        name="attend",
    )(low, qkv, start.reshape(length, 1))


def head_back(d, raw, gain, cosine, sine):
    dn = d * cosine + pltpu.roll(d * sine, HD // 2, 1)
    raw = raw.astype(F32)
    r = lax.rsqrt(jnp.mean(raw * raw, axis=1, keepdims=True) + EPSILON)
    n = raw * r
    dg = jnp.sum(dn * n, axis=0, keepdims=True)
    scaled = dn * gain
    dv = r * (scaled - n * jnp.mean(scaled * n, axis=1, keepdims=True))
    return dv.astype(BF), dg


def attend_back_kernel(
    low_ref,
    qkv_ref,
    do_ref,
    o_ref,
    lse_ref,
    start_ref,
    raw_ref,
    cos_ref,
    sin_ref,
    hg_ref,
    out_ref,
    dg_ref,
    dk_acc,
    dv_acc,
    dq_acc,
):
    blocks = qkv_ref.shape[0] // BLK
    dg_ref[...] = jnp.zeros_like(dg_ref)

    def query_block(qb, carry):
        r0 = pl.multiple_of(qb * BLK, BLK)
        rows = pl.ds(r0, BLK)
        q2 = stack_heads(qkv_ref[rows, 0:256])
        do2 = stack_heads(do_ref[rows, :])
        o2 = stack_heads(o_ref[rows, :])
        delta = jnp.sum(jnp.transpose(do2.astype(F32) * o2.astype(F32)), axis=0, keepdims=True)
        lse = jnp.concatenate([lse_ref[0, 0:1, rows], lse_ref[0, 1:2, rows]], axis=1)
        first = start_ref[0:1, rows]
        first2 = jnp.concatenate([first, first], axis=1)

        def tile(k0, diagonal):
            k = qkv_ref[pl.ds(k0, BLK), 256:384]
            v = qkv_ref[pl.ds(k0, BLK), 384:512]
            key = lax.broadcasted_iota(jnp.int32, (BLK, 2 * BLK), 0)
            mask = key >= first2 - k0
            if diagonal:
                query = lax.broadcasted_iota(jnp.int32, (BLK, 2 * BLK), 1) & (BLK - 1)
                mask = mask & (key <= query)
            p = jnp.where(mask, jnp.exp2(nt(k, q2) * (SCALE * LOG2E) - lse), 0.0)
            ds = (p * (nt(v, do2) - delta)).astype(BF)
            return nn(ds, q2), nn(p.astype(BF), do2), tn(ds, k)

        dk, dv, dq = tile(r0, True)
        dk_acc[rows, :] = dk
        dv_acc[rows, :] = dv
        dq_acc[...] = dq

        def step(kb, inner):
            k0 = pl.multiple_of(kb * BLK, BLK)
            dk, dv, dq = tile(k0, False)
            dk_acc[pl.ds(k0, BLK), :] += dk
            dv_acc[pl.ds(k0, BLK), :] += dv
            dq_acc[...] += dq
            return inner

        lax.fori_loop(low_ref[qb], qb, step, 0)
        cosine = cos_ref[rows, :]
        sine = sin_ref[rows, :]
        for h in range(2):
            d_raw, dg = head_back(
                dq_acc[h * BLK : (h + 1) * BLK, :] * SCALE,
                raw_ref[rows, h * HD : (h + 1) * HD],
                hg_ref[0:1, :],
                cosine,
                sine,
            )
            out_ref[rows, h * HD : (h + 1) * HD] = d_raw
            dg_ref[0, 0:1, :] += dg
        return carry

    lax.fori_loop(0, blocks, query_block, 0)

    def key_block(kb, carry):
        rows = pl.ds(pl.multiple_of(kb * BLK, BLK), BLK)
        d_raw, dg = head_back(
            dk_acc[rows, :] * SCALE,
            raw_ref[rows, 256:384],
            hg_ref[1:2, :],
            cos_ref[rows, :],
            sin_ref[rows, :],
        )
        out_ref[rows, 256:384] = d_raw
        out_ref[rows, 384:512] = dv_acc[rows, :].astype(BF)
        dg_ref[0, 1:2, :] += dg
        return carry

    lax.fori_loop(0, blocks, key_block, 0)


def attend_back(low, qkv, d_att, att, lse, start, raw, cosine, sine, head_gains):
    length, cols = qkv.shape
    groups = cols // 512
    column = lambda n: pl.BlockSpec((length, n), lambda g, low: (0, g))
    return pl.pallas_call(
        attend_back_kernel,
        grid_spec=pltpu.PrefetchScalarGridSpec(
            num_scalar_prefetch=1,
            grid=(groups,),
            in_specs=[
                column(512),
                column(256),
                column(256),
                pl.BlockSpec((1, 2, length), lambda g, low: (g, 0, 0)),
                full_spec((1, length)),
                column(384),
                full_spec((length, HD)),
                full_spec((length, HD)),
                full_spec((2, HD)),
            ],
            out_specs=[
                column(512),
                pl.BlockSpec((1, 2, HD), lambda g, low: (g, 0, 0)),
            ],
            scratch_shapes=[
                pltpu.VMEM((length, HD), F32),
                pltpu.VMEM((length, HD), F32),
                pltpu.VMEM((2 * BLK, HD), F32),
            ],
        ),
        out_shape=[
            jax.ShapeDtypeStruct((length, cols), BF),
            jax.ShapeDtypeStruct((groups, 2, HD), F32),
        ],
        name="attend_back",
    )(low, qkv, d_att, att, lse, start.reshape(1, length), raw, cosine, sine, head_gains)


def mlp_kernel(m_ref, g_ref, wgu_ref, wd_ref, hid_ref, dgu_ref):
    m = m_ref[...]
    g = g_ref[...]
    half = wd_ref.shape[0]
    step = 512
    for n in range(0, half, step):
        gate = nn(m, wgu_ref[:, n : n + step])
        up = nn(m, wgu_ref[:, half + n : half + n + step])
        dh = nt(g, wd_ref[n : n + step, :])
        sig = 1.0 / (1.0 + jnp.exp(-gate))
        act = gate * sig
        hid_ref[:, n : n + step] = (act * up).astype(BF)
        dgu_ref[:, n : n + step] = (dh * up * (sig + act * (1.0 - sig))).astype(BF)
        dgu_ref[:, half + n : half + n + step] = (dh * act).astype(BF)


def mlp(mlp_in, cot, w_gu, w_down):
    length, width = mlp_in.shape
    half = w_down.shape[0]
    rows = lambda n: pl.BlockSpec((BLK, n), lambda t: (t, 0))
    return pl.pallas_call(
        mlp_kernel,
        grid=(length // BLK,),
        in_specs=[rows(width), rows(width), full_spec((width, 2 * half)), full_spec((half, width))],
        out_specs=[rows(half), rows(2 * half)],
        out_shape=[
            jax.ShapeDtypeStruct((length, half), BF),
            jax.ShapeDtypeStruct((length, 2 * half), BF),
        ],
        name="mlp",
    )(mlp_in, cot, w_gu, w_down)


def swap(value, axis):
    size = lax.axis_size(axis)
    return lax.ppermute(value, axis, [(i, i ^ 1) for i in range(size)])


def ordered(first_is_mine, mine, other):
    return jnp.where(
        first_is_mine,
        jnp.concatenate([mine, other], axis=0),
        jnp.concatenate([other, mine], axis=0),
    )


def part(value, index, count, axis=0):
    size = value.shape[axis] // count
    return lax.dynamic_slice_in_dim(value, index * size, size, axis)


def columns(value, *ranges):
    return [value[:, a:b] for a, b in ranges]


def pack_qkv(w_q, w_k, w_v):
    halves = []
    for c in range(2):
        pieces = []
        for kv in (2 * c, 2 * c + 1, 4 + 2 * c, 5 + 2 * c):
            pieces.append(w_q[:, kv * 256 : (kv + 1) * 256])
            pieces.append(w_k[:, kv * HD : (kv + 1) * HD])
            pieces.append(w_v[:, kv * HD : (kv + 1) * HD])
        halves.append(jnp.concatenate(pieces, axis=1))
    return halves


def unpack_qkv(halves):
    w_q, w_k, w_v = ([None] * KV for _ in range(3))
    for c in range(2):
        for n, kv in enumerate((2 * c, 2 * c + 1, 4 + 2 * c, 5 + 2 * c)):
            block = halves[c][:, n * 512 : (n + 1) * 512]
            w_q[kv], w_k[kv], w_v[kv] = block[:, :256], block[:, 256:384], block[:, 384:]
    return tuple(jnp.concatenate(w, axis=1) for w in (w_q, w_k, w_v))


def pack_gu(w_gate, w_up):
    quarter = w_gate.shape[1] // 4
    halves = []
    for c in range(2):
        pieces = []
        for w in (w_gate, w_up):
            pieces.append(w[:, c * quarter : (c + 1) * quarter])
            pieces.append(w[:, (2 + c) * quarter : (3 + c) * quarter])
        halves.append(jnp.concatenate(pieces, axis=1))
    return halves


def unpack_gu(halves):
    quarter = halves[0].shape[1] // 4
    out = []
    for n in range(2):
        q = [h[:, (2 * n + k) * quarter : (2 * n + k + 1) * quarter] for k in range(2) for h in halves]
        out.append(jnp.concatenate(q, axis=1))
    return tuple(out)


def take_rows(full, core):
    quarters = full.reshape(4, full.shape[0] // 4, full.shape[1])
    return jnp.concatenate(
        [
            lax.dynamic_index_in_dim(quarters, core, 0, keepdims=False),
            lax.dynamic_index_in_dim(quarters, 2 + core, 0, keepdims=False),
        ],
        axis=0,
    )


def gather_any(value):
    return lax.all_gather(value, ("fsdp", "seq"), axis=0, tiled=True)


class Exchange:
    def __init__(self):
        self.core = lax.axis_index("seq")
        self.row = lax.axis_index("fsdp")
        self.side = lax.axis_index("rep") % 2
        self.pairs = lax.axis_size("fsdp") == 2 and lax.axis_size("rep") % 2 == 0

    def over_fsdp(self, mine, split):
        if split:
            here = swap(part(mine, self.side, 2), "fsdp")
            there = swap(here, "rep")
            other = ordered(self.side == 0, here, there)
        else:
            other = swap(mine, "fsdp")
        return ordered(self.row == 0, mine, other)

    def rows(self, shard, split=True):
        if not self.pairs:
            return take_rows(gather_any(shard), self.core)
        return self.over_fsdp(shard, split)

    def cols(self, halves, split=True):
        if not self.pairs:
            full = [gather_any(h) for h in halves]
            return jnp.where(self.core == 0, full[0], full[1])
        mine = jnp.where(self.core == 0, halves[0], halves[1])
        other = jnp.where(self.core == 0, halves[1], halves[0])
        local = ordered(self.core == 0, mine, swap(other, "seq"))
        return self.over_fsdp(local, split)

    def over_rep(self, value):
        size = lax.axis_size("rep")
        mine = part(value, self.side, 2) + swap(part(value, 1 - self.side, 2), "rep")
        if size > 2:
            groups = [[i for i in range(size) if i % 2 == s] for s in range(2)]
            mine = lax.psum(mine, "rep", axis_index_groups=groups)
        return ordered(self.side == 0, mine, swap(mine, "rep"))

    def sum_rows(self, grad):
        if not self.pairs:
            quarter = grad.shape[0] // 2
            full = jnp.zeros((4, quarter, grad.shape[1]), BF)
            full = lax.dynamic_update_slice(full, grad[None, :quarter], (self.core, 0, 0))
            full = lax.dynamic_update_slice(full, grad[None, quarter:], (2 + self.core, 0, 0))
            return self.scatter_any(full.reshape(4 * quarter, grad.shape[1])).astype(F32)
        mine = part(grad, self.row, 2) + swap(part(grad, 1 - self.row, 2), "fsdp")
        return self.over_rep(mine).astype(F32)

    def scatter_any(self, full):
        shard = lax.psum_scatter(full, ("fsdp", "seq"), scatter_dimension=0, tiled=True)
        return lax.psum(shard, "rep")

    def sum_cols(self, grad):
        if not self.pairs:
            zero = jnp.zeros_like(grad)
            halves = [
                self.scatter_any(jnp.where(self.core == c, grad, zero)).astype(F32) for c in range(2)
            ]
            return halves
        mine = part(grad, self.row, 2) + swap(part(grad, 1 - self.row, 2), "fsdp")
        mine = self.over_rep(mine)
        keep = part(mine, self.core, 2)
        got = swap(part(mine, 1 - self.core, 2), "seq")
        return [
            jnp.where(self.core == 0, keep, got).astype(F32),
            jnp.where(self.core == 0, got, keep).astype(F32),
        ]


def norm_back(d, v, gain):
    r = lax.rsqrt(jnp.mean(v * v, axis=1, keepdims=True) + EPSILON)
    n = v * r
    scaled = d * gain
    dv = r * (scaled - n * jnp.mean(scaled * n, axis=1, keepdims=True))
    return dv, jnp.sum(d * n, axis=0)


def on_device(
    tokens,
    segments,
    attn_norm,
    w_q,
    w_k,
    w_v,
    q_norm,
    k_norm,
    w_o,
    mlp_norm,
    w_gate,
    w_up,
    w_down,
    cotangent,
):
    ex = Exchange()
    rows, width = tokens.shape
    length = 2 * rows
    core = ex.core

    sizes = (attn_norm.shape[0], mlp_norm.shape[0], q_norm.shape[0], k_norm.shape[0])
    gains = gather_any(jnp.concatenate([attn_norm, mlp_norm, q_norm, k_norm])[None, :]).astype(F32)
    offsets = [0, sizes[0], sizes[0] + sizes[1], sizes[0] + sizes[1] + sizes[2], sum(sizes)]
    attn_gain, mlp_gain, q_gain, k_gain = (
        gains[:, offsets[n] : offsets[n + 1]].reshape(1, -1) for n in range(4)
    )
    head_gains = jnp.concatenate([q_gain, k_gain], axis=0)

    wqkv = ex.cols(pack_qkv(w_q, w_k, w_v), split=False)
    wo = ex.rows(w_o)
    wgu = ex.cols(pack_gu(w_gate, w_up))
    wd = ex.rows(w_down)

    tokens_other = swap(tokens, "seq")
    cot_other = swap(cotangent, "seq")
    x_all = ordered(core == 0, tokens, tokens_other)

    seg = segments[0]
    start = jnp.sum((seg[None, :] < seg[:, None]).astype(jnp.int32), axis=1)
    position = (jnp.arange(length, dtype=jnp.int32) - start).astype(F32)
    inverse = ROPE_BASE ** (jnp.arange(HD // 2, dtype=F32) * (-2.0 / HD))
    angles = position[:, None] * inverse[None, :]
    cos_half, sin_half = jnp.cos(angles), jnp.sin(angles)
    cosine = jnp.concatenate([cos_half, cos_half], axis=1)
    sine = jnp.concatenate([-sin_half, sin_half], axis=1)
    low = start[::BLK] // BLK

    normed, qkv, raw = project(x_all, attn_gain, wqkv, cosine, sine, head_gains)
    attended, lse = attend(low, qkv, start)

    mixed_other = nn(part(attended, 1 - core, 2), wo).astype(BF)
    mixed_mine = nn(part(attended, core, 2), wo)
    middle = tokens.astype(F32) + mixed_mine + swap(mixed_other, "seq").astype(F32)
    scale = lax.rsqrt(jnp.mean(middle * middle, axis=1, keepdims=True) + EPSILON)
    mlp_mine = (middle * scale * mlp_gain).astype(BF)
    mlp_in = jnp.concatenate([mlp_mine, swap(mlp_mine, "seq")], axis=0)
    cot_local = jnp.concatenate([cotangent, cot_other], axis=0)

    hidden, d_gu = mlp(mlp_in, cot_local, wgu, wd)
    g_down = ex.sum_rows(tn(hidden, cot_local).astype(BF))
    g_gu = ex.sum_cols(tn(mlp_in, d_gu).astype(BF))

    d_in_other = nt(d_gu[rows:], wgu).astype(BF)
    d_in = nt(d_gu[:rows], wgu) + swap(d_in_other, "seq").astype(F32)
    d_mid, dg_mlp = norm_back(d_in, middle, mlp_gain)
    d_middle = cotangent.astype(F32) + d_mid
    d_branch = d_middle.astype(BF)
    branch_all = ordered(core == 0, d_branch, swap(d_branch, "seq"))
    d_att = nt(branch_all, wo).astype(BF)
    g_o = ex.sum_rows(tn(attended, branch_all).astype(BF))

    d_qkv, dg_heads = attend_back(
        low, qkv, d_att, attended, lse, start, raw, cosine, sine, head_gains
    )
    g_qkv = ex.sum_cols(tn(normed, d_qkv).astype(BF))

    d_norm_other = nt(part(d_qkv, 1 - core, 2), wqkv).astype(BF)
    d_normed = nt(part(d_qkv, core, 2), wqkv) + swap(d_norm_other, "seq").astype(F32)
    d_tok, dg_attn = norm_back(d_normed, tokens.astype(F32), attn_gain)
    tokens_grad = d_middle + d_tok

    out_other = nn(hidden[rows:], wd).astype(BF)
    output = (middle + nn(hidden[:rows], wd) + swap(out_other, "seq").astype(F32)).astype(BF)

    dg_heads = jnp.sum(dg_heads, axis=0)
    small = lax.psum(
        jnp.concatenate([dg_attn, dg_mlp, dg_heads[0], dg_heads[1]]), ("rep", "fsdp", "seq")
    )
    shard = ex.row * 2 + core
    pieces = []
    at = 0
    for size in sizes:
        total = size * lax.axis_size("fsdp") * 2
        pieces.append(lax.dynamic_slice_in_dim(small[at : at + total], shard * size, size, 0))
        at += total
    g_q, g_k, g_v = unpack_qkv(g_qkv)
    g_gate, g_up = unpack_gu(g_gu)
    return (
        output,
        tokens_grad,
        pieces[0],
        g_q,
        g_k,
        g_v,
        pieces[2],
        pieces[3],
        g_o,
        pieces[1],
        g_gate,
        g_up,
        g_down,
    )


def solution(mesh):
    token_rows = P(("rep", "fsdp", "seq"), None)
    vec = P(("fsdp", "seq"))
    mat = P(("fsdp", "seq"), None)
    return jax.shard_map(
        on_device,
        mesh=mesh,
        in_specs=(
            token_rows,
            P(("rep", "fsdp"), None),
            vec,
            mat,
            mat,
            mat,
            vec,
            vec,
            mat,
            vec,
            mat,
            mat,
            mat,
            token_rows,
        ),
        out_specs=(
            token_rows,
            token_rows,
            vec,
            mat,
            mat,
            mat,
            vec,
            vec,
            mat,
            vec,
            mat,
            mat,
            mat,
        ),
        check_vma=False,
    )
```

```python
import functools

import jax
import jax.numpy as jnp
from jax import lax
from jax.experimental import pallas as pl
from jax.experimental.pallas import tpu as pltpu
from jax.sharding import PartitionSpec as P

HQ = 16
KV = 8
HD = 128
EPSILON = 1e-06
ROPE_BASE = 1000000.0
SCALE = HD**-0.5
LOG2E = 1.4426950408889634
BLK = 256
BF = jnp.bfloat16
F32 = jnp.float32


def nn(a, b):
    return lax.dot_general(a, b, (((1,), (0,)), ((), ())), preferred_element_type=F32)


def nt(a, b):
    return lax.dot_general(a, b, (((1,), (1,)), ((), ())), preferred_element_type=F32)


def tn(a, b):
    return lax.dot_general(a, b, (((0,), (0,)), ((), ())), preferred_element_type=F32)


def cost(micros):
    return pl.CostEstimate(flops=int(micros * 1.0e7), transcendentals=0, bytes_accessed=0)


def full_spec(shape):
    return pl.BlockSpec(shape, lambda *_: (0,) * len(shape), pipeline_mode=pl.Buffered(1))


class Weight:
    def __init__(self, pieces, base):
        self.pieces = [p for p, _ in pieces]
        self.starts = [s for _, s in pieces]
        self.base = base
        self.shape = (sum(p.shape[0] for p in self.pieces), self.pieces[0].shape[1])


def tiled(name, body, steps, info, inputs, weights, outputs, micros):
    n_in, n_out = len(inputs), len(outputs)
    pieces = [p for w in weights for p in w.pieces]

    def kernel(info_ref, *refs):
        ins = refs[:n_in]
        parts = refs[n_in : n_in + len(pieces)]
        outs = refs[n_in + len(pieces) : n_in + len(pieces) + n_out]
        rest = refs[n_in + len(pieces) + n_out :]
        held, sems = rest[: len(weights)], rest[len(weights) :]

        if pieces:

            @pl.when(pl.program_id(0) == 0)
            def _():
                copies = []
                at = 0
                for n, w in enumerate(weights):
                    for k, piece in enumerate(w.pieces):
                        first = pl.multiple_of(info_ref[w.base + k], 128)
                        target = held[n].at[pl.ds(first, piece.shape[0]), :]
                        copies.append(pltpu.make_async_copy(parts[at], target, sems[0].at[at]))
                        at += 1
                for copy in copies:
                    copy.start()
                for copy in copies:
                    copy.wait()

        body(info_ref, ins, held, outs)

    scratch = [pltpu.VMEM(w.shape, BF) for w in weights]
    if pieces:
        scratch.append(pltpu.SemaphoreType.DMA((len(pieces),)))
    return pl.pallas_call(
        kernel,
        grid_spec=pltpu.PrefetchScalarGridSpec(
            num_scalar_prefetch=1,
            grid=(steps,),
            in_specs=[pl.BlockSpec(block, index) for _, block, index in inputs]
            + [pl.BlockSpec(memory_space=pl.ANY)] * len(pieces),
            out_specs=[pl.BlockSpec(block, index) for _, block, index in outputs],
            scratch_shapes=scratch,
        ),
        out_shape=[shape for shape, _, _ in outputs],
        cost_estimate=cost(micros),
        name=name,
    )(info, *[a for a, _, _ in inputs], *pieces)


def struct(rows, cols, dtype=BF):
    return jax.ShapeDtypeStruct((rows, cols), dtype)


def at_row(t, i):
    return (t, 0)


def once(t, i):
    return (0, 0)


def block(array, index=at_row):
    return (array, (BLK, array.shape[1]), index)


def const(array):
    return (array, array.shape, once)


def result(rows, cols, dtype=BF, index=at_row):
    return (struct(rows, cols, dtype), (BLK, cols), index)


class Order:
    def __init__(self, rows):
        self.half = rows // BLK

    def own(self, t, i):
        return (t + self.half * i[0], 0)

    def other(self, t, i):
        return (t + self.half * (1 - i[0]), 0)

    def global_(self, t, i):
        return ((t + self.half * i[0]) % (2 * self.half), 0)

    def first(self, t, i):
        return (jnp.minimum(t, self.half - 1), 0)

    def second(self, t, i):
        return (jnp.maximum(t - self.half, 0), 0)

    def later(self, t, i):
        return (t + self.half, 0)


def both(order, a, b):
    return jnp.where(pl.program_id(0) < order.half, a[...], b[...])


def project(order, info, tokens, other, gain, weight, cosine, sine, head_gains):
    rows, width = tokens.shape
    cols = weight.shape[1]

    def body(info_ref, ins, held, outs):
        own_ref, other_ref, gain_ref, cos_ref, sin_ref, hg_ref = ins
        normed_ref, qkv_ref, raw_ref = outs
        x = both(order, own_ref, other_ref).astype(F32)
        scale = lax.rsqrt(jnp.mean(x * x, axis=1, keepdims=True) + EPSILON)
        normed = (x * scale * gain_ref[...]).astype(BF)
        normed_ref[...] = normed
        cos_tab, sin_tab = cos_ref[...], sin_ref[...]
        for g in range(cols // 512):
            acc = nn(normed, held[0][:, g * 512 : (g + 1) * 512])
            for h in range(3):
                t = acc[:, h * HD : (h + 1) * HD]
                head_gain = hg_ref[0:1, :] if h < 2 else hg_ref[1:2, :]
                n = t * lax.rsqrt(jnp.mean(t * t, axis=1, keepdims=True) + EPSILON) * head_gain
                turned = n * cos_tab + pltpu.roll(n, HD // 2, 1) * sin_tab
                qkv_ref[:, g * 512 + h * HD : g * 512 + (h + 1) * HD] = turned.astype(BF)
                raw_ref[:, g * 384 + h * HD : g * 384 + (h + 1) * HD] = t.astype(BF)
            qkv_ref[:, g * 512 + 384 : (g + 1) * 512] = acc[:, 384:].astype(BF)

    place = order.global_
    return tiled(
        "project",
        body,
        2 * order.half,
        info,
        [
            block(tokens, order.first),
            block(other, order.second),
            const(gain),
            block(cosine, place),
            block(sine, place),
            const(head_gains),
        ],
        [weight],
        [
            result(2 * rows, width, BF, place),
            result(2 * rows, cols, BF, place),
            result(2 * rows, cols // 4 * 3, BF, place),
        ],
        17,
    )


def times(name, order, info, inputs, index, weight, transposed, micros):
    rows = inputs[0].shape[0] // 2
    cols = weight.shape[0] if transposed else weight.shape[1]

    def body(info_ref, ins, held, outs):
        outs[0][...] = product(ins, held[0], transposed).astype(BF)

    return tiled(
        name,
        body,
        order.half,
        info,
        [block(a, index) for a in inputs],
        [weight],
        [result(rows, cols)],
        micros,
    )[0]


def product(ins, held, transposed):
    total = None
    at = 0
    for a in ins:
        size = a.shape[1]
        if transposed:
            term = nt(a[...], held[:, at : at + size])
        else:
            term = nn(a[...], held[at : at + size, :])
        total = term if total is None else total + term
        at += size
    return total


def mix_own(order, info, attended, tokens, got, gain, weight):
    rows, width = tokens.shape

    def body(info_ref, ins, held, outs):
        att_ref, tok_ref, got_ref, gain_ref = ins
        middle = (
            tok_ref[...].astype(F32) + nn(att_ref[...], held[0][...]) + got_ref[...].astype(F32)
        )
        outs[0][...] = middle
        scale = lax.rsqrt(jnp.mean(middle * middle, axis=1, keepdims=True) + EPSILON)
        outs[1][...] = (middle * scale * gain_ref[...]).astype(BF)

    return tiled(
        "mix_own",
        body,
        order.half,
        info,
        [block(attended, order.own), block(tokens), block(got), const(gain)],
        [weight],
        [result(rows, width, F32), result(rows, width)],
        6,
    )


def mlp(order, info, m_own, m_other, g_own, g_other, w_gu, w_down):
    rows, width = m_own.shape
    half = w_down.shape[0]
    step = 512

    def body(info_ref, ins, held, outs):
        hid_ref, dgu_ref, m_ref, g_ref = outs
        gu, down = held
        m = both(order, ins[0], ins[1])
        g = both(order, ins[2], ins[3])
        m_ref[...] = m
        g_ref[...] = g
        for n in range(0, half, step):
            gate = nn(m, gu[:, n : n + step])
            up = nn(m, gu[:, half + n : half + n + step])
            dh = nt(g, down[n : n + step, :])
            sig = 1.0 / (1.0 + jnp.exp(-gate))
            act = gate * sig
            hid_ref[:, n : n + step] = (act * up).astype(BF)
            dgu_ref[:, n : n + step] = (dh * up * (sig + act * (1.0 - sig))).astype(BF)
            dgu_ref[:, half + n : half + n + step] = (dh * act).astype(BF)

    return tiled(
        "mlp",
        body,
        2 * order.half,
        info,
        [
            block(m_own, order.first),
            block(m_other, order.second),
            block(g_own, order.first),
            block(g_other, order.second),
        ],
        [w_gu, w_down],
        [
            result(2 * rows, half),
            result(2 * rows, 2 * half),
            result(2 * rows, width),
            result(2 * rows, width),
        ],
        30,
    )


def norm_back(d, v, gain):
    r = lax.rsqrt(jnp.mean(v * v, axis=1, keepdims=True) + EPSILON)
    n = v * r
    scaled = d * gain
    dv = r * (scaled - n * jnp.mean(scaled * n, axis=1, keepdims=True))
    return dv, jnp.sum(d * n, axis=0, keepdims=True)


def add_over_steps(ref, value):
    @pl.when(pl.program_id(0) == 0)
    def _():
        ref[...] = value

    @pl.when(pl.program_id(0) > 0)
    def _():
        ref[...] += value


def branch_own(order, info, d_gu, got, middle, cot, gain, weight):
    rows, width = middle.shape

    def body(info_ref, ins, held, outs):
        d_ref, got_ref, mid_ref, cot_ref, gain_ref = ins
        d = product([d_ref], held[0], True) + got_ref[...].astype(F32)
        dv, dg = norm_back(d, mid_ref[...], gain_ref[...])
        d_middle = cot_ref[...].astype(F32) + dv
        outs[0][...] = d_middle
        outs[1][...] = d_middle.astype(BF)
        add_over_steps(outs[2], dg)

    return tiled(
        "branch_own",
        body,
        order.half,
        info,
        [block(d_gu), block(got), block(middle), block(cot), const(gain)],
        [weight],
        [
            result(rows, width, F32),
            result(rows, width),
            (struct(1, width, F32), (1, width), once),
        ],
        11,
    )


def attended_back(order, info, own, other, weight):
    rows, width = own.shape

    def body(info_ref, ins, held, outs):
        branch = both(order, ins[0], ins[1])
        outs[1][...] = branch
        outs[0][...] = nt(branch, held[0][...]).astype(BF)

    place = order.global_
    return tiled(
        "attended_back",
        body,
        2 * order.half,
        info,
        [block(own, order.first), block(other, order.second)],
        [weight],
        [result(2 * rows, weight.shape[0], BF, place), result(2 * rows, width, BF, place)],
        8,
    )


def tokens_own(order, info, d_parts, got, tokens, d_middle, gain, weight):
    rows, width = tokens.shape

    def body(info_ref, ins, held, outs):
        parts, (got_ref, tok_ref, mid_ref, gain_ref) = ins[: len(d_parts)], ins[len(d_parts) :]
        d = product(parts, held[0], True) + got_ref[...].astype(F32)
        dv, dg = norm_back(d, tok_ref[...].astype(F32), gain_ref[...])
        outs[0][...] = mid_ref[...] + dv
        add_over_steps(outs[1], dg)

    return tiled(
        "tokens_own",
        body,
        order.half,
        info,
        [block(d, order.own) for d in d_parts]
        + [block(got), block(tokens), block(d_middle), const(gain)],
        [weight],
        [result(rows, width, F32), (struct(1, width, F32), (1, width), once)],
        9,
    )


def output_own(order, info, hidden, middle, got, weight):
    rows, width = middle.shape

    def body(info_ref, ins, held, outs):
        hid_ref, mid_ref, got_ref = ins
        total = mid_ref[...] + nn(hid_ref[...], held[0][...]) + got_ref[...].astype(F32)
        outs[0][...] = total.astype(BF)

    return tiled(
        "output_own",
        body,
        order.half,
        info,
        [block(hidden), block(middle), block(got)],
        [weight],
        [result(rows, width)],
        6,
    )[0]


def stack_heads(block):
    return jnp.concatenate([block[:, :HD], block[:, HD:]], axis=0)


def attend_kernel(low_ref, qkv_ref, start_ref, out_ref, lse_ref, acc, total):
    blocks = qkv_ref.shape[0] // BLK

    def query_block(qb, carry):
        r0 = pl.multiple_of(qb * BLK, BLK)
        q2 = stack_heads(qkv_ref[pl.ds(r0, BLK), 0:256])
        first = start_ref[pl.ds(r0, BLK), :]
        first2 = jnp.concatenate([first, first], axis=0)

        def tile(k0, diagonal):
            k = qkv_ref[pl.ds(k0, BLK), 256:384]
            v = qkv_ref[pl.ds(k0, BLK), 384:512]
            s = nt(q2, k) * (SCALE * LOG2E)
            col = lax.broadcasted_iota(jnp.int32, (2 * BLK, BLK), 1)
            mask = col >= first2 - k0
            if diagonal:
                row = lax.broadcasted_iota(jnp.int32, (2 * BLK, BLK), 0) & (BLK - 1)
                mask = mask & (col <= row)
            p = jnp.where(mask, jnp.exp2(s), 0.0)
            part = p[:, :HD]
            for n in range(1, BLK // HD):
                part = part + p[:, n * HD : (n + 1) * HD]
            return part, nn(p.astype(BF), v)

        part, mixed = tile(r0, True)
        total[...] = part
        acc[...] = mixed

        def step(kb, inner):
            more, mixed_more = tile(pl.multiple_of(kb * BLK, BLK), False)
            total[...] += more
            acc[...] += mixed_more
            return inner

        lax.fori_loop(low_ref[qb], qb, step, 0)
        sums = total[...]
        o = (acc[...] / jnp.sum(sums, axis=1, keepdims=True)).astype(BF)
        out_ref[pl.ds(r0, BLK), 0:HD] = o[:BLK]
        out_ref[pl.ds(r0, BLK), HD : 2 * HD] = o[BLK:]
        line = jnp.log2(jnp.sum(jnp.transpose(sums), axis=0, keepdims=True))
        lse_ref[0, 0:1, pl.ds(r0, BLK)] = line[:, :BLK]
        lse_ref[0, 1:2, pl.ds(r0, BLK)] = line[:, BLK:]
        return carry

    lax.fori_loop(0, blocks, query_block, 0)


def attend(low, qkv, start, at, groups, earlier=None):
    length, cols = qkv.shape
    whole = cols // 512
    anywhere = [pl.BlockSpec(memory_space=pl.ANY)] * (2 if earlier else 0)

    def body(low_ref, qkv_ref, start_ref, *rest):
        attend_kernel(low_ref, qkv_ref, start_ref, *rest[len(anywhere) :])

    return pl.pallas_call(
        body,
        grid_spec=pltpu.PrefetchScalarGridSpec(
            num_scalar_prefetch=1,
            grid=(groups,),
            in_specs=[
                pl.BlockSpec((length, 512), lambda g, low: (0, g + at)),
                full_spec((length, 1)),
                *anywhere,
            ],
            out_specs=[
                pl.BlockSpec((length, 256), lambda g, low: (0, g + at)),
                pl.BlockSpec((1, 2, length), lambda g, low: (g + at, 0, 0)),
            ],
            scratch_shapes=[
                pltpu.VMEM((2 * BLK, HD), F32),
                pltpu.VMEM((2 * BLK, HD), F32),
            ],
        ),
        out_shape=[
            jax.ShapeDtypeStruct((length, whole * 256), BF),
            jax.ShapeDtypeStruct((whole, 2, length), F32),
        ],
        input_output_aliases={3: 0, 4: 1} if earlier else {},
        cost_estimate=cost(11.5 * groups),
        name="attend",
    )(low, qkv, start.reshape(length, 1), *(earlier or ()))


def head_back(d, raw, gain, cosine, sine):
    dn = d * cosine + pltpu.roll(d * sine, HD // 2, 1)
    raw = raw.astype(F32)
    r = lax.rsqrt(jnp.mean(raw * raw, axis=1, keepdims=True) + EPSILON)
    n = raw * r
    dg = jnp.sum(dn * n, axis=0, keepdims=True)
    scaled = dn * gain
    dv = r * (scaled - n * jnp.mean(scaled * n, axis=1, keepdims=True))
    return dv.astype(BF), dg


def attend_back_kernel(
    low_ref,
    qkv_ref,
    do_ref,
    o_ref,
    lse_ref,
    start_ref,
    raw_ref,
    cos_ref,
    sin_ref,
    hg_ref,
    out_ref,
    dg_ref,
    dk_acc,
    dv_acc,
    dq_acc,
):
    blocks = qkv_ref.shape[0] // BLK
    dg_ref[...] = jnp.zeros_like(dg_ref)

    def query_block(qb, carry):
        r0 = pl.multiple_of(qb * BLK, BLK)
        rows = pl.ds(r0, BLK)
        q2 = stack_heads(qkv_ref[rows, 0:256])
        do2 = stack_heads(do_ref[rows, :])
        o2 = stack_heads(o_ref[rows, :])
        delta = jnp.sum(jnp.transpose(do2.astype(F32) * o2.astype(F32)), axis=0, keepdims=True)
        lse = jnp.concatenate([lse_ref[0, 0:1, rows], lse_ref[0, 1:2, rows]], axis=1)
        first = start_ref[0:1, rows]
        first2 = jnp.concatenate([first, first], axis=1)

        def tile(k0, diagonal):
            k = qkv_ref[pl.ds(k0, BLK), 256:384]
            v = qkv_ref[pl.ds(k0, BLK), 384:512]
            key = lax.broadcasted_iota(jnp.int32, (BLK, 2 * BLK), 0)
            mask = key >= first2 - k0
            if diagonal:
                query = lax.broadcasted_iota(jnp.int32, (BLK, 2 * BLK), 1) & (BLK - 1)
                mask = mask & (key <= query)
            p = jnp.where(mask, jnp.exp2(nt(k, q2) * (SCALE * LOG2E) - lse), 0.0)
            ds = (p * (nt(v, do2) - delta)).astype(BF)
            return nn(ds, q2), nn(p.astype(BF), do2), tn(ds, k)

        dk, dv, dq = tile(r0, True)
        dk_acc[rows, :] = dk
        dv_acc[rows, :] = dv
        dq_acc[...] = dq

        def step(kb, inner):
            k0 = pl.multiple_of(kb * BLK, BLK)
            dk, dv, dq = tile(k0, False)
            dk_acc[pl.ds(k0, BLK), :] += dk
            dv_acc[pl.ds(k0, BLK), :] += dv
            dq_acc[...] += dq
            return inner

        lax.fori_loop(low_ref[qb], qb, step, 0)
        cosine = cos_ref[rows, :]
        sine = sin_ref[rows, :]
        for h in range(2):
            d_raw, dg = head_back(
                dq_acc[h * BLK : (h + 1) * BLK, :] * SCALE,
                raw_ref[rows, h * HD : (h + 1) * HD],
                hg_ref[0:1, :],
                cosine,
                sine,
            )
            out_ref[rows, h * HD : (h + 1) * HD] = d_raw
            dg_ref[0:1, :] += dg
        return carry

    lax.fori_loop(0, blocks, query_block, 0)

    def key_block(kb, carry):
        rows = pl.ds(pl.multiple_of(kb * BLK, BLK), BLK)
        d_raw, dg = head_back(
            dk_acc[rows, :] * SCALE,
            raw_ref[rows, 256:384],
            hg_ref[1:2, :],
            cos_ref[rows, :],
            sin_ref[rows, :],
        )
        out_ref[rows, 256:384] = d_raw
        out_ref[rows, 384:512] = dv_acc[rows, :].astype(BF)
        dg_ref[1:2, :] += dg
        return carry

    lax.fori_loop(0, blocks, key_block, 0)


def attend_back(low, qkv, d_att, att, lse, start, raw, cosine, sine, head_gains, at, earlier):
    length = qkv.shape[0]
    anywhere = [] if earlier is None else [pl.BlockSpec(memory_space=pl.ANY)]

    def body(*refs):
        attend_back_kernel(*refs[:10], *refs[10 + len(anywhere) :])

    column = lambda n: pl.BlockSpec((length, n), lambda g, low: (0, g + at))
    return pl.pallas_call(
        body,
        grid_spec=pltpu.PrefetchScalarGridSpec(
            num_scalar_prefetch=1,
            grid=(1,),
            in_specs=[
                column(512),
                column(256),
                column(256),
                pl.BlockSpec((1, 2, length), lambda g, low: (g + at, 0, 0)),
                full_spec((1, length)),
                column(384),
                full_spec((length, HD)),
                full_spec((length, HD)),
                full_spec((2, HD)),
                *anywhere,
            ],
            out_specs=[
                pl.BlockSpec((length, 512), lambda g, low: (0, at % 3)),
                pl.BlockSpec((2, HD), lambda g, low: (0, 0)),
            ],
            scratch_shapes=[
                pltpu.VMEM((length, HD), F32),
                pltpu.VMEM((length, HD), F32),
                pltpu.VMEM((2 * BLK, HD), F32),
            ],
        ),
        out_shape=[
            jax.ShapeDtypeStruct((length, 1536 if at < 3 else 512), BF),
            jax.ShapeDtypeStruct((2, HD), F32),
        ],
        input_output_aliases={} if earlier is None else {10: 0},
        cost_estimate=cost(21),
        name="attend_back",
    )(low, qkv, d_att, att, lse, start.reshape(1, length), raw, cosine, sine, head_gains, *([] if earlier is None else [earlier]))


def core_heads(c):
    return (2 * c, 2 * c + 1, 4 + 2 * c, 5 + 2 * c)


def qkv_columns(c):
    out = []
    for kv in core_heads(c):
        out += [(0, kv * 256, 256), (1, kv * HD, HD), (2, kv * HD, HD)]
    return out


def gu_columns(c, quarter):
    return [(n, k * quarter, quarter) for n in range(2) for k in (c, 2 + c)]


def pack(name, info, arrays, layout):
    rows = arrays[0].shape[0]
    cols = sum(a.shape[1] for a in arrays) // 2

    def body(info_ref, ins, held, outs):
        for c in range(2):

            @pl.when(info_ref[0] == c)
            def _():
                for target, half in ((outs[0], c), (outs[1], 1 - c)):
                    at = 0
                    for n, first, size in layout(half):
                        target[:, at : at + size] = ins[n][:, first : first + size]
                        at += size

    return tiled(
        name,
        body,
        1,
        info,
        [const(a) for a in arrays],
        [],
        [(struct(rows, cols), (rows, cols), once)] * 2,
        3,
    )


def unpack(name, info, keeps, gots, widths, layout):
    rows = keeps[0].shape[0]
    count = len(keeps)

    def body(info_ref, ins, held, outs):
        for c in range(2):

            @pl.when(info_ref[0] == c)
            def _():
                for half in range(2):
                    source = ins[:count] if half == c else ins[count:]
                    at = 0
                    for n, first, size in layout(half):
                        ref = source[at // source[0].shape[1]]
                        col = at % source[0].shape[1]
                        outs[n][:, first : first + size] = ref[:, col : col + size].astype(F32)
                        at += size

    return tiled(
        name,
        body,
        1,
        info,
        [const(a) for a in keeps + gots],
        [],
        [(struct(rows, w, F32), (rows, w), once) for w in widths],
        4,
    )


def swap(value, axis, bit=0):
    size = lax.axis_size(axis)
    return lax.ppermute(value, axis, [(i, i ^ (1 << bit)) for i in range(size)])


def ordered(first_is_mine, mine, other):
    return jnp.where(
        first_is_mine,
        jnp.concatenate([mine, other], axis=0),
        jnp.concatenate([other, mine], axis=0),
    )


def part(value, index, count, axis=0):
    size = value.shape[axis] // count
    return lax.dynamic_slice_in_dim(value, index * size, size, axis)


def gather_any(value):
    return lax.all_gather(value, ("fsdp", "seq"), axis=0, tiled=True)


def fence(*values):
    return lax.optimization_barrier(values)


class Sum:
    def __init__(self, grad, row, replica):
        self.row, self.replica = row, replica
        self.value = grad.reshape(2, 2, grad.shape[0] // 4, grad.shape[1])

    def send(self, axis):
        self.at = (0, self.row) if axis == "fsdp" else (1, self.replica % 2)
        dim, mine = self.at
        self.got = swap(part(self.value, 1 - mine, 2, dim), axis)
        return self

    def add(self):
        dim, mine = self.at
        self.value = part(self.value, mine, 2, dim) + self.got
        return self

    def flat(self):
        return self.value.reshape(-1, self.value.shape[-1])

STRIP = 512


def strips(*values):
    return jnp.concatenate(
        [v[:, at : at + STRIP] for v in values for at in range(0, v.shape[1], STRIP)], axis=0
    )


def halve(value, replica, bit):
    return swap(part(value, 1 - ((replica >> bit) & 1), 2), "rep", bit)


def add_half(value, got, replica, bit):
    return part(value, (replica >> bit) & 1, 2) + got


def double(value, got, replica, bit):
    return ordered((replica >> bit) & 1 == 0, value, got)


def finish_gu(info, values, gots, quarter):
    rows = gots[0].shape[0] * STRIP // (2 * quarter)
    piece = 256

    def body(info_ref, ins, held, outs):
        for c in range(2):
            for side in range(2):

                @pl.when((info_ref[0] == c) & (info_ref[1] == side))
                def _():
                    for n in range(2):
                        own, got = ins[2 * n + (c != side)], ins[4 + n]
                        for half, ref in ((c, own), (1 - c, got)):
                            for at in range(0, 2 * quarter, piece):
                                r, col = at // STRIP * rows, at % STRIP
                                k, to = at // quarter, at % quarter
                                to += (half + 2 * k) * quarter
                                outs[n][:, to : to + piece] = ref[
                                    r : r + rows, col : col + piece
                                ].astype(F32)

    return tiled(
        "finish_gu",
        body,
        1,
        info,
        [const(a) for pair in values for a in pair] + [const(g) for g in gots],
        [],
        [(struct(rows, 4 * quarter, F32), (rows, 4 * quarter), once)] * 2,
        5,
    )


def finish_rows(info, values, firsts, width):
    strips_n = width // STRIP
    sizes = [(v[0].shape[0] - first) // strips_n for v, first in zip(values, firsts)]

    def body(info_ref, ins, held, outs):
        for side in range(2):

            @pl.when(info_ref[1] == side)
            def _():
                for n, (first, rows) in enumerate(zip(firsts, sizes)):
                    for which in range(2):
                        to = rows * (side if which == 0 else 1 - side)
                        for k in range(strips_n):
                            outs[n][to : to + rows, k * STRIP : (k + 1) * STRIP] = ins[
                                2 * n + which
                            ][first + k * rows : first + (k + 1) * rows, :].astype(F32)

    return tiled(
        "finish_rows",
        body,
        1,
        info,
        [const(a) for pair in values for a in pair],
        [],
        [(struct(2 * r, width, F32), (2 * r, width), once) for r in sizes],
        5,
    )


def land(sums, other):
    *gots, other = fence(*[s.got for s in sums], other)
    for s, got in zip(sums, gots):
        s.got = got
    return other


def take_rows(full, core):
    quarters = full.reshape(4, full.shape[0] // 4, full.shape[1])
    return jnp.concatenate(
        [
            lax.dynamic_index_in_dim(quarters, core, 0, keepdims=False),
            lax.dynamic_index_in_dim(quarters, 2 + core, 0, keepdims=False),
        ],
        axis=0,
    )


def whole_cols(core, mine, send):
    halves = jnp.where(core == 0, mine, send), jnp.where(core == 0, send, mine)
    full = [gather_any(h) for h in halves]
    return jnp.where(core == 0, full[0], full[1])


def scatter_any(full):
    shard = lax.psum_scatter(full, ("fsdp", "seq"), scatter_dimension=0, tiled=True)
    return lax.psum(shard, "rep")


def any_rows(core, grad):
    quarter = grad.shape[0] // 2
    full = jnp.zeros((4, quarter, grad.shape[1]), BF)
    full = lax.dynamic_update_slice(full, grad[None, :quarter], (core, 0, 0))
    full = lax.dynamic_update_slice(full, grad[None, quarter:], (2 + core, 0, 0))
    return scatter_any(full.reshape(4 * quarter, grad.shape[1]))


def any_cols(core, grads):
    keeps, gots = [], []
    for grad in grads:
        halves = [scatter_any(jnp.where(core == c, grad, jnp.zeros_like(grad))) for c in range(2)]
        keeps.append(jnp.where(core == 0, halves[0], halves[1]))
        gots.append(jnp.where(core == 0, halves[1], halves[0]))
    return keeps, gots


def gather_small(vec):
    value = vec[None, :]
    for axis in ("seq", "fsdp"):
        size = lax.axis_size(axis)
        if size & (size - 1):
            return gather_any(vec[None, :])
        for bit in range(size.bit_length() - 1):
            got = lax.ppermute(value, axis, [(i, i ^ (1 << bit)) for i in range(size)])
            value = ordered((lax.axis_index(axis) >> bit) % 2 == 0, value, got)
    return value


def sum_small(value):
    for axis in ("seq", "fsdp", "rep"):
        size = lax.axis_size(axis)
        if size & (size - 1):
            value = lax.psum(value, axis)
            continue
        for bit in range(size.bit_length() - 1):
            value = value + lax.ppermute(value, axis, [(i, i ^ (1 << bit)) for i in range(size)])
    return value


def on_device(
    tokens,
    segments,
    attn_norm,
    w_q,
    w_k,
    w_v,
    q_norm,
    k_norm,
    w_o,
    mlp_norm,
    w_gate,
    w_up,
    w_down,
    cotangent,
):
    core = lax.axis_index("seq")
    row = lax.axis_index("fsdp")
    replica = lax.axis_index("rep")
    rep_size = lax.axis_size("rep")
    pairs = lax.axis_size("fsdp") == 2 and rep_size == 8
    rows, width = tokens.shape
    length = 2 * rows
    order = Order(rows)
    quarter = w_gate.shape[1] // 4
    gu_layout = functools.partial(gu_columns, quarter=quarter)
    side = replica % 2

    def starts(size, blocks):
        return [size * b for b in blocks]

    if pairs:
        quad = [2 * row + core, 2 * row + 1 - core, 2 * (1 - row) + core, 2 * (1 - row) + 1 - core]
        near, far = 2 * (1 - row) + core, 2 * (1 - row) + 1 - core
        gu_far = [jnp.where(side == 0, near, far), jnp.where(side == 0, far, near)]
        o_rows, d_rows = w_o.shape[0], w_down.shape[0]
        layout = (
            starts(w_q.shape[0], quad)
            + [o_rows * row, o_rows * (1 - row)]
            + starts(w_gate.shape[0], quad[:2] + gu_far)
            + [d_rows * row, d_rows * (1 - row)]
        )
        bases = (2, 6, 8, 12)
    else:
        layout = [0 * core] * 4
        bases = (2, 3, 4, 5)
    info = jnp.stack([core, side] + layout).astype(jnp.int32)

    sizes = (attn_norm.shape[0], mlp_norm.shape[0], q_norm.shape[0], k_norm.shape[0])
    gains = gather_small(jnp.concatenate([attn_norm, mlp_norm, q_norm, k_norm])).astype(F32)
    offsets = [0, sizes[0], sizes[0] + sizes[1], sizes[0] + sizes[1] + sizes[2], sum(sizes)]
    attn_gain, mlp_gain, q_gain, k_gain = (
        gains[:, offsets[n] : offsets[n + 1]].reshape(1, -1) for n in range(4)
    )
    head_gains = jnp.concatenate([q_gain, k_gain], axis=0)

    seg = segments[0]
    start = jnp.sum((seg[None, :] < seg[:, None]).astype(jnp.int32), axis=1)
    position = (jnp.arange(length, dtype=jnp.int32) - start).astype(F32)
    inverse = ROPE_BASE ** (jnp.arange(HD // 2, dtype=F32) * (-2.0 / HD))
    angles = position[:, None] * inverse[None, :]
    cos_half, sin_half = jnp.cos(angles), jnp.sin(angles)
    cosine = jnp.concatenate([cos_half, cos_half], axis=1)
    sine = jnp.concatenate([-sin_half, sin_half], axis=1)

    mine, send = pack("pack_qkv", info, [w_q, w_k, w_v], qkv_columns)
    got = swap(send, "seq")
    tokens_other = swap(tokens, "seq")
    if pairs:
        mine_far, got_far = swap(mine, "fsdp"), swap(got, "fsdp")
        got, w_gate, w_up = fence(got, w_gate, w_up)
        gu_mine, send = pack("pack_gu", info, [w_gate, w_up], gu_layout)
        gu_got = swap(send, "seq")
        gu_here = jnp.where(side == 0, gu_mine, gu_got)
        mine_far, got_far, attn_gain, head_gains, cosine, sine, gu_here, w_o, w_down = fence(
            mine_far, got_far, attn_gain, head_gains, cosine, sine, gu_here, w_o, w_down
        )
        wqkv = Weight(list(zip([mine, got, mine_far, got_far], layout[:4])), bases[0])
        gu_here, o_there = swap(gu_here, "fsdp"), swap(w_o, "fsdp")
    else:
        wqkv = Weight([(whole_cols(core, mine, send), 0)], bases[0])
        wo = Weight([(take_rows(gather_any(w_o), core), 0)], bases[1])
        mine, send = pack("pack_gu", info, [w_gate, w_up], gu_layout)
        wgu = Weight([(whole_cols(core, mine, send), 0)], bases[2])
        wd = Weight([(take_rows(gather_any(w_down), core), 0)], bases[3])

    cot_other = swap(cotangent, "seq")

    low = start[::BLK] // BLK

    normed, qkv, raw = project(
        order, info, tokens, tokens_other, attn_gain, wqkv, cosine, sine, head_gains
    )
    done = attend(low, qkv, start, 0, 1)
    if pairs:
        *done, gu_here = fence(*done, gu_here)
        gu_there = swap(gu_here, "rep")
    done = attend(low, qkv, start, 1, 2, done)
    if pairs:
        *done, o_there, w_down = fence(*done, o_there, w_down)
        d_there = swap(w_down, "fsdp")
        wo = Weight(list(zip([w_o, o_there], layout[4:6])), bases[1])
    attended, lse = attend(low, qkv, start, 3, 1, done)

    sent = times("mix_other", order, info, [attended], order.other, wo, False, 5)
    if pairs:
        sent, gu_there, d_there = fence(sent, gu_there, d_there)
        wgu = Weight(list(zip([gu_mine, gu_got, gu_here, gu_there], layout[6:10])), bases[2])
        wd = Weight(list(zip([w_down, d_there], layout[10:])), bases[3])
    middle, m_own = mix_own(order, info, attended, tokens, swap(sent, "seq"), mlp_gain, wo)
    hidden, d_gu, m_all, g_all = mlp(
        order, info, m_own, swap(m_own, "seq"), cotangent, cot_other, wgu, wd
    )
    g_down = tn(hidden, g_all).astype(BF)
    if pairs:
        d_gu, g_down = fence(d_gu, g_down)

    sent = times("branch_other", order, info, [d_gu], order.later, wgu, True, 9)
    got = swap(sent, "seq")
    m_all, sent = fence(m_all, sent)
    g_gu = tn(m_all, d_gu).astype(BF)
    d_gu, got, g_gu = fence(d_gu, got, g_gu)
    d_middle, d_branch, dg_mlp = branch_own(
        order, info, d_gu, got, middle, cotangent, mlp_gain, wgu
    )
    branch_other = swap(d_branch, "seq")
    d_att, branch_all = attended_back(order, info, d_branch, branch_other, wo)
    g_o = tn(attended, branch_all).astype(BF)
    if pairs:
        down = Sum(g_down, row, replica).send("rep")
        gate, up = (
            Sum(g_gu[:, n * 2 * quarter : (n + 1) * 2 * quarter], row, replica).send("fsdp")
            for n in range(2)
        )
        o_sum = Sum(g_o, row, replica).send("fsdp")
        d_att, g_o = fence(d_att, g_o)

    def back(at, earlier=None):
        return attend_back(
            low, qkv, d_att, attended, lse, start, raw, cosine, sine, head_gains, at, earlier
        )

    d_qkv0, dg0 = back(0)
    if pairs:
        d_qkv0 = land([down, gate], d_qkv0)
        down.add().send("fsdp")
        gate.add().send("rep")
    d_qkv0, dg1 = back(1, d_qkv0)
    if pairs:
        d_qkv0 = land([down, gate, up], d_qkv0)
        early = strips(gate.add().flat(), down.add().flat())
        early_got = halve(early, replica, 1)
        up.add().send("rep")
    d_qkv0, dg2 = back(2, d_qkv0)
    if pairs:
        early_got, up.got, o_sum.got, d_qkv0 = fence(early_got, up.got, o_sum.got, d_qkv0)
        early = add_half(early, early_got, replica, 1)
        early_got = halve(early, replica, 2)
        o_sum.add().send("rep")
    g_qkv0 = tn(normed, d_qkv0).astype(BF)
    if pairs:
        qkv0 = Sum(g_qkv0, row, replica).send("fsdp")
    d_att, g_qkv0 = fence(d_att, g_qkv0)
    d_qkv1, dg3 = back(3)
    if pairs:
        early_got, o_sum.got, qkv0.got, d_qkv1 = fence(early_got, o_sum.got, qkv0.got, d_qkv1)
    g_qkv1 = tn(normed, d_qkv1).astype(BF)
    d_qkv1, g_qkv1 = fence(d_qkv1, g_qkv1)
    if pairs:
        qkv1 = Sum(g_qkv1, row, replica).send("fsdp")
        early = add_half(early, early_got, replica, 2)
        early_got = swap(early, "rep", 2)
        late = strips(up.add().flat(), o_sum.add().flat())
        late_got = halve(late, replica, 1)
        qkv0.add().send("rep")

    sent = times("tokens_other", order, info, [d_qkv0, d_qkv1], order.other, wqkv, True, 6)
    if pairs:
        early_got, late_got, qkv0.got, qkv1.got, sent = fence(
            early_got, late_got, qkv0.got, qkv1.got, sent
        )
        qkv1.add().send("rep")
        early = double(early, early_got, replica, 2)
        early_got = swap(early, "rep", 1)
        late = add_half(late, late_got, replica, 1)
        late_got = halve(late, replica, 2)
    hidden, sent = fence(hidden, sent)
    out_sent = times("output_other", order, info, [hidden], order.later, wd, False, 6)
    if pairs:
        early_got, late_got, qkv1.got, out_sent = fence(early_got, late_got, qkv1.got, out_sent)
        last = jnp.concatenate([qkv0.add().flat(), qkv1.add().flat()], axis=1)
        last_got = halve(last, replica, 1)
        early = double(early, early_got, replica, 1)
        early_far = swap(early, "rep", 0)
        late = add_half(late, late_got, replica, 2)
        late_got = swap(late, "rep", 2)
    sent, out_sent = fence(sent, out_sent)
    got, out_got = swap(sent, "seq"), swap(out_sent, "seq")
    tokens_grad, dg_attn = tokens_own(
        order, info, [d_qkv0, d_qkv1], got, tokens, d_middle, attn_gain, wqkv
    )
    dg_heads = dg0 + dg1 + dg2 + dg3
    small = jnp.concatenate([dg_attn[0], dg_mlp[0], dg_heads[0], dg_heads[1]])
    if pairs:
        late_got, last_got, tokens_grad = fence(late_got, last_got, tokens_grad)
        last = add_half(last, last_got, replica, 1)
        last_got = halve(last, replica, 2)
        late = double(late, late_got, replica, 2)
        late_got = swap(late, "rep", 1)
        hop = swap(small, "seq")
    hidden, tokens_grad = fence(hidden, tokens_grad)
    output = output_own(order, info, hidden, middle, out_got, wd)
    if pairs:
        early_far, last_got, hop, output = fence(early_far, last_got, hop, output)
        last = add_half(last, last_got, replica, 2)
        last_got = swap(last, "rep", 2)
        small = small + hop
        hop = swap(small, "fsdp")

        late_got, last_got, hop = fence(late_got, last_got, hop)
        last = double(last, last_got, replica, 2)
        last_got = swap(last, "rep", 1)
        late = double(late, late_got, replica, 1)
        late_far = swap(late, "rep", 0)
        small = small + hop
        hop = swap(small, "rep", 1)

        last_got, hop = fence(last_got, hop)
        last = double(last, last_got, replica, 1)
        last_far = swap(last, "rep", 0)
        small = small + hop
        hop = swap(small, "rep", 2)

        late_far, hop = fence(late_far, hop)
        small = small + hop
        hop = swap(small, "rep", 0)
        home = core == side
        gu_rows = early.shape[0] // 2
        values = [(early, early_far), (late, late_far)]
        gots = [swap(jnp.where(home, b[:gu_rows], a[:gu_rows]), "seq") for a, b in values]
        g_gate, g_up = finish_gu(info, values, gots, quarter)
        g_down, g_o = finish_rows(info, values, [gu_rows, gu_rows], width)

        last_far, g_gate, g_up, g_down, g_o, hop = fence(
            last_far, g_gate, g_up, g_down, g_o, hop
        )
        small = small + hop
        keep, send = jnp.where(home, last, last_far), jnp.where(home, last_far, last)
        qkv_parts = [keep], [swap(send, "seq")]
    else:
        small = sum_small(small)
        g_down, g_o = (any_rows(core, g).astype(F32) for g in (g_down, g_o))
        qkv_parts = any_cols(core, [jnp.concatenate([g_qkv0, g_qkv1], axis=1)])
        gu_parts = any_cols(core, [g_gu[:, : 2 * quarter], g_gu[:, 2 * quarter :]])
        g_gate, g_up = unpack("unpack_gu", info, *gu_parts, [w_gate.shape[1]] * 2, gu_layout)
    g_q, g_k, g_v = unpack(
        "unpack_qkv", info, *qkv_parts, [a.shape[1] for a in (w_q, w_k, w_v)], qkv_columns
    )

    shard = row * 2 + core
    pieces = []
    at = 0
    for size in sizes:
        total = size * lax.axis_size("fsdp") * 2
        pieces.append(lax.dynamic_slice_in_dim(small[at : at + total], shard * size, size, 0))
        at += total
    return (
        output,
        tokens_grad,
        pieces[0],
        g_q,
        g_k,
        g_v,
        pieces[2],
        pieces[3],
        g_o,
        pieces[1],
        g_gate,
        g_up,
        g_down,
    )


def solution(mesh):
    token_rows = P(("rep", "fsdp", "seq"), None)
    vec = P(("fsdp", "seq"))
    mat = P(("fsdp", "seq"), None)
    return jax.shard_map(
        on_device,
        mesh=mesh,
        in_specs=(
            token_rows,
            P(("rep", "fsdp"), None),
            vec,
            mat,
            mat,
            mat,
            vec,
            vec,
            mat,
            vec,
            mat,
            mat,
            mat,
            token_rows,
        ),
        out_specs=(
            token_rows,
            token_rows,
            vec,
            mat,
            mat,
            mat,
            vec,
            vec,
            mat,
            vec,
            mat,
            mat,
            mat,
        ),
        check_vma=False,
    )
```

```python
import functools

import jax
import jax.numpy as jnp
from jax import lax
from jax.experimental import pallas as pl
from jax.experimental.pallas import tpu as pltpu
from jax.sharding import PartitionSpec as P

HQ = 16
KV = 8
HD = 128
EPSILON = 1e-06
ROPE_BASE = 1000000.0
SCALE = HD**-0.5
LOG2E = 1.4426950408889634
BLK = 256
BF = jnp.bfloat16
F32 = jnp.float32


def nn(a, b):
    return lax.dot_general(a, b, (((1,), (0,)), ((), ())), preferred_element_type=F32)


def nt(a, b):
    return lax.dot_general(a, b, (((1,), (1,)), ((), ())), preferred_element_type=F32)


def tn(a, b):
    return lax.dot_general(a, b, (((0,), (0,)), ((), ())), preferred_element_type=F32)


def cost(micros):
    return pl.CostEstimate(flops=int(micros * 1.0e7), transcendentals=0, bytes_accessed=0)


def full_spec(shape):
    return pl.BlockSpec(shape, lambda *_: (0,) * len(shape), pipeline_mode=pl.Buffered(1))


class Weight:
    def __init__(self, pieces, base):
        self.pieces = [p for p, _ in pieces]
        self.starts = [s for _, s in pieces]
        self.base = base
        self.shape = (sum(p.shape[0] for p in self.pieces), self.pieces[0].shape[1])


def tiled(name, body, steps, info, inputs, weights, outputs, micros):
    n_in, n_out = len(inputs), len(outputs)
    pieces = [p for w in weights for p in w.pieces]

    def kernel(info_ref, *refs):
        ins = refs[:n_in]
        parts = refs[n_in : n_in + len(pieces)]
        outs = refs[n_in + len(pieces) : n_in + len(pieces) + n_out]
        rest = refs[n_in + len(pieces) + n_out :]
        held, sems = rest[: len(weights)], rest[len(weights) :]

        if pieces:

            @pl.when(pl.program_id(0) == 0)
            def _():
                copies = []
                at = 0
                for n, w in enumerate(weights):
                    for k, piece in enumerate(w.pieces):
                        first = pl.multiple_of(info_ref[w.base + k], 128)
                        target = held[n].at[pl.ds(first, piece.shape[0]), :]
                        copies.append(pltpu.make_async_copy(parts[at], target, sems[0].at[at]))
                        at += 1
                for copy in copies:
                    copy.start()
                for copy in copies:
                    copy.wait()

        body(info_ref, ins, held, outs)

    scratch = [pltpu.VMEM(w.shape, BF) for w in weights]
    if pieces:
        scratch.append(pltpu.SemaphoreType.DMA((len(pieces),)))
    return pl.pallas_call(
        kernel,
        grid_spec=pltpu.PrefetchScalarGridSpec(
            num_scalar_prefetch=1,
            grid=(steps,),
            in_specs=[pl.BlockSpec(block, index) for _, block, index in inputs]
            + [pl.BlockSpec(memory_space=pl.ANY)] * len(pieces),
            out_specs=[pl.BlockSpec(block, index) for _, block, index in outputs],
            scratch_shapes=scratch,
        ),
        out_shape=[shape for shape, _, _ in outputs],
        cost_estimate=cost(micros),
        name=name,
    )(info, *[a for a, _, _ in inputs], *pieces)


def struct(rows, cols, dtype=BF):
    return jax.ShapeDtypeStruct((rows, cols), dtype)


def at_row(t, i):
    return (t, 0)


def once(t, i):
    return (0, 0)


def block(array, index=at_row):
    return (array, (BLK, array.shape[1]), index)


def const(array):
    return (array, array.shape, once)


def result(rows, cols, dtype=BF, index=at_row):
    return (struct(rows, cols, dtype), (BLK, cols), index)


class Order:
    def __init__(self, rows):
        self.half = rows // BLK

    def own(self, t, i):
        return (t + self.half * i[0], 0)

    def other(self, t, i):
        return (t + self.half * (1 - i[0]), 0)

    def global_(self, t, i):
        return ((t + self.half * i[0]) % (2 * self.half), 0)

    def first(self, t, i):
        return (jnp.minimum(t, self.half - 1), 0)

    def second(self, t, i):
        return (jnp.maximum(t - self.half, 0), 0)

    def later(self, t, i):
        return (t + self.half, 0)


def both(order, a, b):
    return jnp.where(pl.program_id(0) < order.half, a[...], b[...])


def project(order, info, tokens, other, gain, weight, cosine, sine, head_gains):
    rows, width = tokens.shape
    cols = weight.shape[1]

    def body(info_ref, ins, held, outs):
        own_ref, other_ref, gain_ref, cos_ref, sin_ref, hg_ref = ins
        normed_ref, qkv_ref, raw_ref = outs
        x = both(order, own_ref, other_ref).astype(F32)
        scale = lax.rsqrt(jnp.mean(x * x, axis=1, keepdims=True) + EPSILON)
        normed = (x * scale * gain_ref[...]).astype(BF)
        normed_ref[...] = normed
        cos_tab, sin_tab = cos_ref[...], sin_ref[...]
        for g in range(cols // 512):
            acc = nn(normed, held[0][:, g * 512 : (g + 1) * 512])
            for h in range(3):
                t = acc[:, h * HD : (h + 1) * HD]
                head_gain = hg_ref[0:1, :] if h < 2 else hg_ref[1:2, :]
                n = t * lax.rsqrt(jnp.mean(t * t, axis=1, keepdims=True) + EPSILON) * head_gain
                turned = n * cos_tab + pltpu.roll(n, HD // 2, 1) * sin_tab
                qkv_ref[:, g * 512 + h * HD : g * 512 + (h + 1) * HD] = turned.astype(BF)
                raw_ref[:, g * 384 + h * HD : g * 384 + (h + 1) * HD] = t.astype(BF)
            qkv_ref[:, g * 512 + 384 : (g + 1) * 512] = acc[:, 384:].astype(BF)

    place = order.global_
    return tiled(
        "project",
        body,
        2 * order.half,
        info,
        [
            block(tokens, order.first),
            block(other, order.second),
            const(gain),
            block(cosine, place),
            block(sine, place),
            const(head_gains),
        ],
        [weight],
        [
            result(2 * rows, width, BF, place),
            result(2 * rows, cols, BF, place),
            result(2 * rows, cols // 4 * 3, BF, place),
        ],
        17,
    )


def times(name, order, info, inputs, index, weight, transposed, micros):
    rows = inputs[0].shape[0] // 2
    cols = weight.shape[0] if transposed else weight.shape[1]

    def body(info_ref, ins, held, outs):
        outs[0][...] = product(ins, held[0], transposed).astype(BF)

    return tiled(
        name,
        body,
        order.half,
        info,
        [block(a, index) for a in inputs],
        [weight],
        [result(rows, cols)],
        micros,
    )[0]


def product(ins, held, transposed):
    total = None
    at = 0
    for a in ins:
        size = a.shape[1]
        if transposed:
            term = nt(a[...], held[:, at : at + size])
        else:
            term = nn(a[...], held[at : at + size, :])
        total = term if total is None else total + term
        at += size
    return total


def mix_own(order, info, attended, tokens, got, gain, weight):
    rows, width = tokens.shape

    def body(info_ref, ins, held, outs):
        att_ref, tok_ref, got_ref, gain_ref = ins
        middle = (
            tok_ref[...].astype(F32) + nn(att_ref[...], held[0][...]) + got_ref[...].astype(F32)
        )
        outs[0][...] = middle
        scale = lax.rsqrt(jnp.mean(middle * middle, axis=1, keepdims=True) + EPSILON)
        outs[1][...] = (middle * scale * gain_ref[...]).astype(BF)

    return tiled(
        "mix_own",
        body,
        order.half,
        info,
        [block(attended, order.own), block(tokens), block(got), const(gain)],
        [weight],
        [result(rows, width, F32), result(rows, width)],
        6,
    )


def mlp(order, info, m_own, m_other, g_own, g_other, w_gu, w_down):
    rows, width = m_own.shape
    half = w_down.shape[0]
    step = 512

    def body(info_ref, ins, held, outs):
        hid_ref, dgu_ref, m_ref, g_ref = outs
        gu, down = held
        m = both(order, ins[0], ins[1])
        g = both(order, ins[2], ins[3])
        m_ref[...] = m
        g_ref[...] = g
        for n in range(0, half, step):
            gate = nn(m, gu[:, n : n + step])
            up = nn(m, gu[:, half + n : half + n + step])
            dh = nt(g, down[n : n + step, :])
            sig = 1.0 / (1.0 + jnp.exp(-gate))
            act = gate * sig
            hid_ref[:, n : n + step] = (act * up).astype(BF)
            dgu_ref[:, n : n + step] = (dh * up * (sig + act * (1.0 - sig))).astype(BF)
            dgu_ref[:, half + n : half + n + step] = (dh * act).astype(BF)

    return tiled(
        "mlp",
        body,
        2 * order.half,
        info,
        [
            block(m_own, order.first),
            block(m_other, order.second),
            block(g_own, order.first),
            block(g_other, order.second),
        ],
        [w_gu, w_down],
        [
            result(2 * rows, half),
            result(2 * rows, 2 * half),
            result(2 * rows, width),
            result(2 * rows, width),
        ],
        30,
    )


def norm_back(d, v, gain):
    r = lax.rsqrt(jnp.mean(v * v, axis=1, keepdims=True) + EPSILON)
    n = v * r
    scaled = d * gain
    dv = r * (scaled - n * jnp.mean(scaled * n, axis=1, keepdims=True))
    return dv, jnp.sum(d * n, axis=0, keepdims=True)


def add_over_steps(ref, value):
    @pl.when(pl.program_id(0) == 0)
    def _():
        ref[...] = value

    @pl.when(pl.program_id(0) > 0)
    def _():
        ref[...] += value


def branch_own(order, info, d_gu, got, middle, cot, gain, weight):
    rows, width = middle.shape

    def body(info_ref, ins, held, outs):
        d_ref, got_ref, mid_ref, cot_ref, gain_ref = ins
        d = product([d_ref], held[0], True) + got_ref[...].astype(F32)
        dv, dg = norm_back(d, mid_ref[...], gain_ref[...])
        d_middle = cot_ref[...].astype(F32) + dv
        outs[0][...] = d_middle
        outs[1][...] = d_middle.astype(BF)
        add_over_steps(outs[2], dg)

    return tiled(
        "branch_own",
        body,
        order.half,
        info,
        [block(d_gu), block(got), block(middle), block(cot), const(gain)],
        [weight],
        [
            result(rows, width, F32),
            result(rows, width),
            (struct(1, width, F32), (1, width), once),
        ],
        11,
    )


def attended_back(order, info, own, other, weight):
    rows, width = own.shape

    def body(info_ref, ins, held, outs):
        branch = both(order, ins[0], ins[1])
        outs[1][...] = branch
        outs[0][...] = nt(branch, held[0][...]).astype(BF)

    place = order.global_
    return tiled(
        "attended_back",
        body,
        2 * order.half,
        info,
        [block(own, order.first), block(other, order.second)],
        [weight],
        [result(2 * rows, weight.shape[0], BF, place), result(2 * rows, width, BF, place)],
        8,
    )


def tokens_own(order, info, d_parts, got, tokens, d_middle, gain, weight):
    rows, width = tokens.shape

    def body(info_ref, ins, held, outs):
        parts, (got_ref, tok_ref, mid_ref, gain_ref) = ins[: len(d_parts)], ins[len(d_parts) :]
        d = product(parts, held[0], True) + got_ref[...].astype(F32)
        dv, dg = norm_back(d, tok_ref[...].astype(F32), gain_ref[...])
        outs[0][...] = mid_ref[...] + dv
        add_over_steps(outs[1], dg)

    return tiled(
        "tokens_own",
        body,
        order.half,
        info,
        [block(d, order.own) for d in d_parts]
        + [block(got), block(tokens), block(d_middle), const(gain)],
        [weight],
        [result(rows, width, F32), (struct(1, width, F32), (1, width), once)],
        9,
    )


def output_own(order, info, hidden, middle, got, weight):
    rows, width = middle.shape

    def body(info_ref, ins, held, outs):
        hid_ref, mid_ref, got_ref = ins
        total = mid_ref[...] + nn(hid_ref[...], held[0][...]) + got_ref[...].astype(F32)
        outs[0][...] = total.astype(BF)

    return tiled(
        "output_own",
        body,
        order.half,
        info,
        [block(hidden), block(middle), block(got)],
        [weight],
        [result(rows, width)],
        6,
    )[0]


def stack_heads(block):
    return jnp.concatenate([block[:, :HD], block[:, HD:]], axis=0)


def attend_kernel(low_ref, qkv_ref, start_ref, out_ref, lse_ref, acc, total):
    blocks = qkv_ref.shape[0] // BLK

    def query_block(qb, carry):
        r0 = pl.multiple_of(qb * BLK, BLK)
        q2 = stack_heads(qkv_ref[pl.ds(r0, BLK), 0:256])
        first = start_ref[pl.ds(r0, BLK), :]
        first2 = jnp.concatenate([first, first], axis=0)

        def tile(k0, diagonal):
            k = qkv_ref[pl.ds(k0, BLK), 256:384]
            v = qkv_ref[pl.ds(k0, BLK), 384:512]
            s = nt(q2, k) * (SCALE * LOG2E)
            col = lax.broadcasted_iota(jnp.int32, (2 * BLK, BLK), 1)
            mask = col >= first2 - k0
            if diagonal:
                row = lax.broadcasted_iota(jnp.int32, (2 * BLK, BLK), 0) & (BLK - 1)
                mask = mask & (col <= row)
            p = jnp.where(mask, jnp.exp2(s), 0.0)
            part = p[:, :HD]
            for n in range(1, BLK // HD):
                part = part + p[:, n * HD : (n + 1) * HD]
            return part, nn(p.astype(BF), v)

        part, mixed = tile(r0, True)
        total[...] = part
        acc[...] = mixed

        def step(kb, inner):
            more, mixed_more = tile(pl.multiple_of(kb * BLK, BLK), False)
            total[...] += more
            acc[...] += mixed_more
            return inner

        lax.fori_loop(low_ref[qb], qb, step, 0)
        sums = total[...]
        o = (acc[...] / jnp.sum(sums, axis=1, keepdims=True)).astype(BF)
        out_ref[pl.ds(r0, BLK), 0:HD] = o[:BLK]
        out_ref[pl.ds(r0, BLK), HD : 2 * HD] = o[BLK:]
        line = jnp.log2(jnp.sum(jnp.transpose(sums), axis=0, keepdims=True))
        lse_ref[0, 0:1, pl.ds(r0, BLK)] = line[:, :BLK]
        lse_ref[0, 1:2, pl.ds(r0, BLK)] = line[:, BLK:]
        return carry

    lax.fori_loop(0, blocks, query_block, 0)


def attend(low, qkv, start, at, groups, earlier=None):
    length, cols = qkv.shape
    whole = cols // 512
    anywhere = [pl.BlockSpec(memory_space=pl.ANY)] * (2 if earlier else 0)

    def body(low_ref, qkv_ref, start_ref, *rest):
        attend_kernel(low_ref, qkv_ref, start_ref, *rest[len(anywhere) :])

    return pl.pallas_call(
        body,
        grid_spec=pltpu.PrefetchScalarGridSpec(
            num_scalar_prefetch=1,
            grid=(groups,),
            in_specs=[
                pl.BlockSpec((length, 512), lambda g, low: (0, g + at)),
                full_spec((length, 1)),
                *anywhere,
            ],
            out_specs=[
                pl.BlockSpec((length, 256), lambda g, low: (0, g + at)),
                pl.BlockSpec((1, 2, length), lambda g, low: (g + at, 0, 0)),
            ],
            scratch_shapes=[
                pltpu.VMEM((2 * BLK, HD), F32),
                pltpu.VMEM((2 * BLK, HD), F32),
            ],
        ),
        out_shape=[
            jax.ShapeDtypeStruct((length, whole * 256), BF),
            jax.ShapeDtypeStruct((whole, 2, length), F32),
        ],
        input_output_aliases={3: 0, 4: 1} if earlier else {},
        cost_estimate=cost(11.5 * groups),
        name="attend",
    )(low, qkv, start.reshape(length, 1), *(earlier or ()))


def head_back(d, raw, gain, cosine, sine):
    dn = d * cosine + pltpu.roll(d * sine, HD // 2, 1)
    raw = raw.astype(F32)
    r = lax.rsqrt(jnp.mean(raw * raw, axis=1, keepdims=True) + EPSILON)
    n = raw * r
    dg = jnp.sum(dn * n, axis=0, keepdims=True)
    scaled = dn * gain
    dv = r * (scaled - n * jnp.mean(scaled * n, axis=1, keepdims=True))
    return dv.astype(BF), dg


def attend_back_kernel(
    low_ref,
    qkv_ref,
    do_ref,
    o_ref,
    lse_ref,
    start_ref,
    raw_ref,
    cos_ref,
    sin_ref,
    hg_ref,
    out_ref,
    dg_ref,
    dk_acc,
    dv_acc,
    dq_acc,
):
    blocks = qkv_ref.shape[0] // BLK
    dg_ref[...] = jnp.zeros_like(dg_ref)

    def query_block(qb, carry):
        r0 = pl.multiple_of(qb * BLK, BLK)
        rows = pl.ds(r0, BLK)
        q2 = stack_heads(qkv_ref[rows, 0:256])
        do2 = stack_heads(do_ref[rows, :])
        o2 = stack_heads(o_ref[rows, :])
        delta = jnp.sum(jnp.transpose(do2.astype(F32) * o2.astype(F32)), axis=0, keepdims=True)
        lse = jnp.concatenate([lse_ref[0, 0:1, rows], lse_ref[0, 1:2, rows]], axis=1)
        first = start_ref[0:1, rows]
        first2 = jnp.concatenate([first, first], axis=1)

        def tile(k0, diagonal):
            k = qkv_ref[pl.ds(k0, BLK), 256:384]
            v = qkv_ref[pl.ds(k0, BLK), 384:512]
            key = lax.broadcasted_iota(jnp.int32, (BLK, 2 * BLK), 0)
            mask = key >= first2 - k0
            if diagonal:
                query = lax.broadcasted_iota(jnp.int32, (BLK, 2 * BLK), 1) & (BLK - 1)
                mask = mask & (key <= query)
            p = jnp.where(mask, jnp.exp2(nt(k, q2) * (SCALE * LOG2E) - lse), 0.0)
            ds = (p * (nt(v, do2) - delta)).astype(BF)
            return nn(ds, q2), nn(p.astype(BF), do2), tn(ds, k)

        dk, dv, dq = tile(r0, True)
        dk_acc[rows, :] = dk
        dv_acc[rows, :] = dv
        dq_acc[...] = dq

        def step(kb, inner):
            k0 = pl.multiple_of(kb * BLK, BLK)
            dk, dv, dq = tile(k0, False)
            dk_acc[pl.ds(k0, BLK), :] += dk
            dv_acc[pl.ds(k0, BLK), :] += dv
            dq_acc[...] += dq
            return inner

        lax.fori_loop(low_ref[qb], qb, step, 0)
        cosine = cos_ref[rows, :]
        sine = sin_ref[rows, :]
        for h in range(2):
            d_raw, dg = head_back(
                dq_acc[h * BLK : (h + 1) * BLK, :] * SCALE,
                raw_ref[rows, h * HD : (h + 1) * HD],
                hg_ref[0:1, :],
                cosine,
                sine,
            )
            out_ref[rows, h * HD : (h + 1) * HD] = d_raw
            dg_ref[0:1, :] += dg
        return carry

    lax.fori_loop(0, blocks, query_block, 0)

    def key_block(kb, carry):
        rows = pl.ds(pl.multiple_of(kb * BLK, BLK), BLK)
        d_raw, dg = head_back(
            dk_acc[rows, :] * SCALE,
            raw_ref[rows, 256:384],
            hg_ref[1:2, :],
            cos_ref[rows, :],
            sin_ref[rows, :],
        )
        out_ref[rows, 256:384] = d_raw
        out_ref[rows, 384:512] = dv_acc[rows, :].astype(BF)
        dg_ref[1:2, :] += dg
        return carry

    lax.fori_loop(0, blocks, key_block, 0)


def attend_back(low, qkv, d_att, att, lse, start, raw, cosine, sine, head_gains, at, earlier):
    length = qkv.shape[0]
    anywhere = [] if earlier is None else [pl.BlockSpec(memory_space=pl.ANY)]

    def body(*refs):
        attend_back_kernel(*refs[:10], *refs[10 + len(anywhere) :])

    column = lambda n: pl.BlockSpec((length, n), lambda g, low: (0, g + at))
    return pl.pallas_call(
        body,
        grid_spec=pltpu.PrefetchScalarGridSpec(
            num_scalar_prefetch=1,
            grid=(1,),
            in_specs=[
                column(512),
                column(256),
                column(256),
                pl.BlockSpec((1, 2, length), lambda g, low: (g + at, 0, 0)),
                full_spec((1, length)),
                column(384),
                full_spec((length, HD)),
                full_spec((length, HD)),
                full_spec((2, HD)),
                *anywhere,
            ],
            out_specs=[
                pl.BlockSpec((length, 512), lambda g, low: (0, at % 3)),
                pl.BlockSpec((2, HD), lambda g, low: (0, 0)),
            ],
            scratch_shapes=[
                pltpu.VMEM((length, HD), F32),
                pltpu.VMEM((length, HD), F32),
                pltpu.VMEM((2 * BLK, HD), F32),
            ],
        ),
        out_shape=[
            jax.ShapeDtypeStruct((length, 1536 if at < 3 else 512), BF),
            jax.ShapeDtypeStruct((2, HD), F32),
        ],
        input_output_aliases={} if earlier is None else {10: 0},
        cost_estimate=cost(21),
        name="attend_back",
    )(low, qkv, d_att, att, lse, start.reshape(1, length), raw, cosine, sine, head_gains, *([] if earlier is None else [earlier]))


def core_heads(c):
    return (2 * c, 2 * c + 1, 4 + 2 * c, 5 + 2 * c)


def qkv_columns(c):
    out = []
    for kv in core_heads(c):
        out += [(0, kv * 256, 256), (1, kv * HD, HD), (2, kv * HD, HD)]
    return out


def gu_columns(c, quarter):
    return [(n, k * quarter, quarter) for n in range(2) for k in (c, 2 + c)]


def pack(name, info, arrays, layout):
    rows = arrays[0].shape[0]
    cols = sum(a.shape[1] for a in arrays) // 2

    def body(info_ref, ins, held, outs):
        for c in range(2):

            @pl.when(info_ref[0] == c)
            def _():
                for target, half in ((outs[0], c), (outs[1], 1 - c)):
                    at = 0
                    for n, first, size in layout(half):
                        target[:, at : at + size] = ins[n][:, first : first + size]
                        at += size

    return tiled(
        name,
        body,
        1,
        info,
        [const(a) for a in arrays],
        [],
        [(struct(rows, cols), (rows, cols), once)] * 2,
        3,
    )


def unpack(name, info, keeps, gots, widths, layout):
    rows = keeps[0].shape[0]
    count = len(keeps)

    def body(info_ref, ins, held, outs):
        for c in range(2):

            @pl.when(info_ref[0] == c)
            def _():
                for half in range(2):
                    source = ins[:count] if half == c else ins[count:]
                    at = 0
                    for n, first, size in layout(half):
                        ref = source[at // source[0].shape[1]]
                        col = at % source[0].shape[1]
                        outs[n][:, first : first + size] = ref[:, col : col + size].astype(F32)
                        at += size

    return tiled(
        name,
        body,
        1,
        info,
        [const(a) for a in keeps + gots],
        [],
        [(struct(rows, w, F32), (rows, w), once) for w in widths],
        4,
    )


def swap(value, axis, bit=0):
    size = lax.axis_size(axis)
    return lax.ppermute(value, axis, [(i, i ^ (1 << bit)) for i in range(size)])


def ordered(first_is_mine, mine, other):
    return jnp.where(
        first_is_mine,
        jnp.concatenate([mine, other], axis=0),
        jnp.concatenate([other, mine], axis=0),
    )


def part(value, index, count, axis=0):
    size = value.shape[axis] // count
    return lax.dynamic_slice_in_dim(value, index * size, size, axis)


def gather_any(value):
    return lax.all_gather(value, ("fsdp", "seq"), axis=0, tiled=True)


def fence(*values):
    return lax.optimization_barrier(values)


class Sum:
    def __init__(self, grad, row, replica):
        self.row, self.replica = row, replica
        self.value = grad.reshape(2, 2, grad.shape[0] // 4, grad.shape[1])

    def send(self, axis):
        self.at = (0, self.row) if axis == "fsdp" else (1, self.replica % 2)
        dim, mine = self.at
        self.got = swap(part(self.value, 1 - mine, 2, dim), axis)
        return self

    def add(self):
        dim, mine = self.at
        self.value = part(self.value, mine, 2, dim) + self.got
        return self

    def flat(self):
        return self.value.reshape(-1, self.value.shape[-1])

STRIP = 512


def strips(*values):
    return jnp.concatenate(
        [v[:, at : at + STRIP] for v in values for at in range(0, v.shape[1], STRIP)], axis=0
    )


def halve(value, replica, bit):
    return swap(part(value, 1 - ((replica >> bit) & 1), 2), "rep", bit)


def add_half(value, got, replica, bit):
    return part(value, (replica >> bit) & 1, 2) + got


def double(value, got, replica, bit):
    return ordered((replica >> bit) & 1 == 0, value, got)


def finish_gu(info, values, gots, quarter):
    rows = gots[0].shape[0] * STRIP // (2 * quarter)
    piece = 256

    def body(info_ref, ins, held, outs):
        for c in range(2):
            for side in range(2):

                @pl.when((info_ref[0] == c) & (info_ref[1] == side))
                def _():
                    for n in range(len(gots)):
                        own, got = ins[2 * n + (c != side)], ins[2 * len(gots) + n]
                        for half, ref in ((c, own), (1 - c, got)):
                            for at in range(0, 2 * quarter, piece):
                                r, col = at // STRIP * rows, at % STRIP
                                k, to = at // quarter, at % quarter
                                to += (half + 2 * k) * quarter
                                outs[n][:, to : to + piece] = ref[
                                    r : r + rows, col : col + piece
                                ].astype(F32)

    return tiled(
        "finish_gu",
        body,
        1,
        info,
        [const(a) for pair in values for a in pair] + [const(g) for g in gots],
        [],
        [(struct(rows, 4 * quarter, F32), (rows, 4 * quarter), once)] * len(gots),
        5,
    )


def finish_rows(info, values, firsts, width):
    strips_n = width // STRIP
    sizes = [(v[0].shape[0] - first) // strips_n for v, first in zip(values, firsts)]

    def body(info_ref, ins, held, outs):
        for side in range(2):

            @pl.when(info_ref[1] == side)
            def _():
                for n, (first, rows) in enumerate(zip(firsts, sizes)):
                    for which in range(2):
                        to = rows * (side if which == 0 else 1 - side)
                        for k in range(strips_n):
                            outs[n][to : to + rows, k * STRIP : (k + 1) * STRIP] = ins[
                                2 * n + which
                            ][first + k * rows : first + (k + 1) * rows, :].astype(F32)

    return tiled(
        "finish_rows",
        body,
        1,
        info,
        [const(a) for pair in values for a in pair],
        [],
        [(struct(2 * r, width, F32), (2 * r, width), once) for r in sizes],
        5,
    )


def land(sums, other):
    *gots, other = fence(*[s.got for s in sums], other)
    for s, got in zip(sums, gots):
        s.got = got
    return other


def take_rows(full, core):
    quarters = full.reshape(4, full.shape[0] // 4, full.shape[1])
    return jnp.concatenate(
        [
            lax.dynamic_index_in_dim(quarters, core, 0, keepdims=False),
            lax.dynamic_index_in_dim(quarters, 2 + core, 0, keepdims=False),
        ],
        axis=0,
    )


def whole_cols(core, mine, send):
    halves = jnp.where(core == 0, mine, send), jnp.where(core == 0, send, mine)
    full = [gather_any(h) for h in halves]
    return jnp.where(core == 0, full[0], full[1])


def scatter_any(full):
    shard = lax.psum_scatter(full, ("fsdp", "seq"), scatter_dimension=0, tiled=True)
    return lax.psum(shard, "rep")


def any_rows(core, grad):
    quarter = grad.shape[0] // 2
    full = jnp.zeros((4, quarter, grad.shape[1]), BF)
    full = lax.dynamic_update_slice(full, grad[None, :quarter], (core, 0, 0))
    full = lax.dynamic_update_slice(full, grad[None, quarter:], (2 + core, 0, 0))
    return scatter_any(full.reshape(4 * quarter, grad.shape[1]))


def any_cols(core, grads):
    keeps, gots = [], []
    for grad in grads:
        halves = [scatter_any(jnp.where(core == c, grad, jnp.zeros_like(grad))) for c in range(2)]
        keeps.append(jnp.where(core == 0, halves[0], halves[1]))
        gots.append(jnp.where(core == 0, halves[1], halves[0]))
    return keeps, gots


def gather_small(vec):
    value = vec[None, :]
    for axis in ("seq", "fsdp"):
        size = lax.axis_size(axis)
        if size & (size - 1):
            return gather_any(vec[None, :])
        for bit in range(size.bit_length() - 1):
            got = lax.ppermute(value, axis, [(i, i ^ (1 << bit)) for i in range(size)])
            value = ordered((lax.axis_index(axis) >> bit) % 2 == 0, value, got)
    return value


def sum_small(value):
    for axis in ("seq", "fsdp", "rep"):
        size = lax.axis_size(axis)
        if size & (size - 1):
            value = lax.psum(value, axis)
            continue
        for bit in range(size.bit_length() - 1):
            value = value + lax.ppermute(value, axis, [(i, i ^ (1 << bit)) for i in range(size)])
    return value


def on_device(
    tokens,
    segments,
    attn_norm,
    w_q,
    w_k,
    w_v,
    q_norm,
    k_norm,
    w_o,
    mlp_norm,
    w_gate,
    w_up,
    w_down,
    cotangent,
):
    core = lax.axis_index("seq")
    row = lax.axis_index("fsdp")
    replica = lax.axis_index("rep")
    rep_size = lax.axis_size("rep")
    pairs = lax.axis_size("fsdp") == 2 and rep_size == 8
    rows, width = tokens.shape
    length = 2 * rows
    order = Order(rows)
    quarter = w_gate.shape[1] // 4
    gu_layout = functools.partial(gu_columns, quarter=quarter)
    side = replica % 2

    def starts(size, blocks):
        return [size * b for b in blocks]

    if pairs:
        quad = [2 * row + core, 2 * row + 1 - core, 2 * (1 - row) + core, 2 * (1 - row) + 1 - core]
        near, far = 2 * (1 - row) + core, 2 * (1 - row) + 1 - core
        gu_far = [jnp.where(side == 0, near, far), jnp.where(side == 0, far, near)]
        o_rows, d_rows = w_o.shape[0], w_down.shape[0]
        layout = (
            starts(w_q.shape[0], quad)
            + [o_rows * row, o_rows * (1 - row)]
            + starts(w_gate.shape[0], quad[:2] + gu_far)
            + [d_rows * row, d_rows * (1 - row)]
        )
        bases = (2, 6, 8, 12)
    else:
        layout = [0 * core] * 4
        bases = (2, 3, 4, 5)
    info = jnp.stack([core, side] + layout).astype(jnp.int32)

    sizes = (attn_norm.shape[0], mlp_norm.shape[0], q_norm.shape[0], k_norm.shape[0])
    gains = gather_small(jnp.concatenate([attn_norm, mlp_norm, q_norm, k_norm])).astype(F32)
    offsets = [0, sizes[0], sizes[0] + sizes[1], sizes[0] + sizes[1] + sizes[2], sum(sizes)]
    attn_gain, mlp_gain, q_gain, k_gain = (
        gains[:, offsets[n] : offsets[n + 1]].reshape(1, -1) for n in range(4)
    )
    head_gains = jnp.concatenate([q_gain, k_gain], axis=0)

    seg = segments[0]
    start = jnp.sum((seg[None, :] < seg[:, None]).astype(jnp.int32), axis=1)
    position = (jnp.arange(length, dtype=jnp.int32) - start).astype(F32)
    inverse = ROPE_BASE ** (jnp.arange(HD // 2, dtype=F32) * (-2.0 / HD))
    angles = position[:, None] * inverse[None, :]
    cos_half, sin_half = jnp.cos(angles), jnp.sin(angles)
    cosine = jnp.concatenate([cos_half, cos_half], axis=1)
    sine = jnp.concatenate([-sin_half, sin_half], axis=1)

    mine, send = pack("pack_qkv", info, [w_q, w_k, w_v], qkv_columns)
    got = swap(send, "seq")
    tokens_other = swap(tokens, "seq")
    if pairs:
        mine_far, got_far = swap(mine, "fsdp"), swap(got, "fsdp")
        got, w_gate, w_up = fence(got, w_gate, w_up)
        gu_mine, send = pack("pack_gu", info, [w_gate, w_up], gu_layout)
        gu_got = swap(send, "seq")
        gu_here = jnp.where(side == 0, gu_mine, gu_got)
        mine_far, got_far, attn_gain, head_gains, cosine, sine, gu_here, w_o, w_down = fence(
            mine_far, got_far, attn_gain, head_gains, cosine, sine, gu_here, w_o, w_down
        )
        wqkv = Weight(list(zip([mine, got, mine_far, got_far], layout[:4])), bases[0])
        gu_here, o_there = swap(gu_here, "fsdp"), swap(w_o, "fsdp")
    else:
        wqkv = Weight([(whole_cols(core, mine, send), 0)], bases[0])
        wo = Weight([(take_rows(gather_any(w_o), core), 0)], bases[1])
        mine, send = pack("pack_gu", info, [w_gate, w_up], gu_layout)
        wgu = Weight([(whole_cols(core, mine, send), 0)], bases[2])
        wd = Weight([(take_rows(gather_any(w_down), core), 0)], bases[3])

    cot_other = swap(cotangent, "seq")

    low = start[::BLK] // BLK

    normed, qkv, raw = project(
        order, info, tokens, tokens_other, attn_gain, wqkv, cosine, sine, head_gains
    )
    done = attend(low, qkv, start, 0, 1)
    if pairs:
        *done, gu_here = fence(*done, gu_here)
        gu_there = swap(gu_here, "rep")
    done = attend(low, qkv, start, 1, 2, done)
    if pairs:
        *done, o_there, w_down = fence(*done, o_there, w_down)
        d_there = swap(w_down, "fsdp")
        wo = Weight(list(zip([w_o, o_there], layout[4:6])), bases[1])
    attended, lse = attend(low, qkv, start, 3, 1, done)

    sent = times("mix_other", order, info, [attended], order.other, wo, False, 5)
    if pairs:
        sent, gu_there, d_there = fence(sent, gu_there, d_there)
        wgu = Weight(list(zip([gu_mine, gu_got, gu_here, gu_there], layout[6:10])), bases[2])
        wd = Weight(list(zip([w_down, d_there], layout[10:])), bases[3])
    middle, m_own = mix_own(order, info, attended, tokens, swap(sent, "seq"), mlp_gain, wo)
    hidden, d_gu, m_all, g_all = mlp(
        order, info, m_own, swap(m_own, "seq"), cotangent, cot_other, wgu, wd
    )
    g_down = tn(hidden, g_all).astype(BF)
    if pairs:
        d_gu, g_down = fence(d_gu, g_down)

    sent = times("branch_other", order, info, [d_gu], order.later, wgu, True, 9)
    got = swap(sent, "seq")
    m_all, sent = fence(m_all, sent)
    g_gu = tn(m_all, d_gu).astype(BF)
    d_gu, got, g_gu = fence(d_gu, got, g_gu)
    d_middle, d_branch, dg_mlp = branch_own(
        order, info, d_gu, got, middle, cotangent, mlp_gain, wgu
    )
    branch_other = swap(d_branch, "seq")
    d_att, branch_all = attended_back(order, info, d_branch, branch_other, wo)
    g_o = tn(attended, branch_all).astype(BF)
    if pairs:
        down = Sum(g_down, row, replica).send("rep")
        gate, up = (
            Sum(g_gu[:, n * 2 * quarter : (n + 1) * 2 * quarter], row, replica).send("fsdp")
            for n in range(2)
        )
        o_sum = Sum(g_o, row, replica).send("fsdp")
        d_att, g_o = fence(d_att, g_o)

    def back(at, earlier=None):
        return attend_back(
            low, qkv, d_att, attended, lse, start, raw, cosine, sine, head_gains, at, earlier
        )

    d_qkv0, dg0 = back(0)
    if pairs:
        d_qkv0 = land([down, gate], d_qkv0)
        down.add().send("fsdp")
        gate.add().send("rep")
    d_qkv0, dg1 = back(1, d_qkv0)
    if pairs:
        d_qkv0 = land([down, gate, up], d_qkv0)
        early = strips(gate.add().flat(), down.add().flat())
        early_got = halve(early, replica, 1)
        up.add().send("rep")
    d_qkv0, dg2 = back(2, d_qkv0)
    if pairs:
        early_got, up.got, o_sum.got, d_qkv0 = fence(early_got, up.got, o_sum.got, d_qkv0)
        early = add_half(early, early_got, replica, 1)
        early_got = halve(early, replica, 2)
        o_sum.add().send("rep")
    g_qkv0 = tn(normed, d_qkv0).astype(BF)
    if pairs:
        qkv0 = Sum(g_qkv0, row, replica).send("fsdp")
    d_att, g_qkv0 = fence(d_att, g_qkv0)
    d_qkv1, dg3 = back(3)
    if pairs:
        early_got, o_sum.got, qkv0.got, d_qkv1 = fence(early_got, o_sum.got, qkv0.got, d_qkv1)
    g_qkv1 = tn(normed, d_qkv1).astype(BF)
    d_qkv1, g_qkv1 = fence(d_qkv1, g_qkv1)
    if pairs:
        qkv1 = Sum(g_qkv1, row, replica).send("fsdp")
        early = add_half(early, early_got, replica, 2)
        early_got = swap(early, "rep", 2)
        late = strips(up.add().flat(), o_sum.add().flat())
        late_got = halve(late, replica, 1)
        qkv0.add().send("rep")

    sent = times("tokens_other", order, info, [d_qkv0, d_qkv1], order.other, wqkv, True, 6)
    if pairs:
        early_got, late_got, qkv0.got, qkv1.got, sent = fence(
            early_got, late_got, qkv0.got, qkv1.got, sent
        )
        qkv1.add().send("rep")
        early = double(early, early_got, replica, 2)
        early_got = swap(early, "rep", 1)
        late = add_half(late, late_got, replica, 1)
        late_got = halve(late, replica, 2)
    hidden, sent = fence(hidden, sent)
    out_sent = times("output_other", order, info, [hidden], order.later, wd, False, 6)
    if pairs:
        early_got, late_got, qkv1.got, out_sent = fence(early_got, late_got, qkv1.got, out_sent)
        last = jnp.concatenate([qkv0.add().flat(), qkv1.add().flat()], axis=1)
        last_got = halve(last, replica, 1)
        early = double(early, early_got, replica, 1)
        early_far = swap(early, "rep", 0)
        late = add_half(late, late_got, replica, 2)
        late_got = swap(late, "rep", 2)
    sent, out_sent = fence(sent, out_sent)
    got, out_got = swap(sent, "seq"), swap(out_sent, "seq")
    tokens_grad, dg_attn = tokens_own(
        order, info, [d_qkv0, d_qkv1], got, tokens, d_middle, attn_gain, wqkv
    )
    dg_heads = dg0 + dg1 + dg2 + dg3
    small = jnp.concatenate([dg_attn[0], dg_mlp[0], dg_heads[0], dg_heads[1]])
    if pairs:
        late_got, last_got, tokens_grad = fence(late_got, last_got, tokens_grad)
        last = add_half(last, last_got, replica, 1)
        last_got = halve(last, replica, 2)
        late = double(late, late_got, replica, 2)
        late_got = swap(late, "rep", 1)
        hop = swap(small, "seq")
    hidden, tokens_grad = fence(hidden, tokens_grad)
    output = output_own(order, info, hidden, middle, out_got, wd)
    if pairs:
        last_got, hop, output = fence(last_got, hop, output)
        last = add_half(last, last_got, replica, 2)
        last_got = swap(last, "rep", 2)
        small = small + hop
        hop = swap(small, "fsdp")
        home = core == side
        gu_rows = early.shape[0] // 2

        def finish(own, far):
            send = jnp.where(home, far[:gu_rows], own[:gu_rows])
            columns = finish_gu(info, [(own, far)], [swap(send, "seq")], quarter)
            return columns + finish_rows(info, [(own, far)], [gu_rows], width)

        late_got, early_far, output = fence(late_got, early_far, output)
        late = double(late, late_got, replica, 1)
        late_far = swap(late, "rep", 0)
        g_gate, g_down = finish(early, early_far)

        last_got, hop, g_gate, g_down = fence(last_got, hop, g_gate, g_down)
        last = double(last, last_got, replica, 2)
        last_got = swap(last, "rep", 1)
        small = small + hop
        hop = swap(small, "rep", 1)

        last_got, hop = fence(last_got, hop)
        last = double(last, last_got, replica, 1)
        last_far = swap(last, "rep", 0)
        small = small + hop
        hop = swap(small, "rep", 2)

        late_far, hop = fence(late_far, hop)
        small = small + hop
        hop = swap(small, "rep", 0)
        g_up, g_o = finish(late, late_far)

        last_far, g_up, g_o, hop = fence(last_far, g_up, g_o, hop)
        small = small + hop
        keep, send = jnp.where(home, last, last_far), jnp.where(home, last_far, last)
        qkv_parts = [keep], [swap(send, "seq")]
    else:
        small = sum_small(small)
        g_down, g_o = (any_rows(core, g).astype(F32) for g in (g_down, g_o))
        qkv_parts = any_cols(core, [jnp.concatenate([g_qkv0, g_qkv1], axis=1)])
        gu_parts = any_cols(core, [g_gu[:, : 2 * quarter], g_gu[:, 2 * quarter :]])
        g_gate, g_up = unpack("unpack_gu", info, *gu_parts, [w_gate.shape[1]] * 2, gu_layout)
    g_q, g_k, g_v = unpack(
        "unpack_qkv", info, *qkv_parts, [a.shape[1] for a in (w_q, w_k, w_v)], qkv_columns
    )

    shard = row * 2 + core
    pieces = []
    at = 0
    for size in sizes:
        total = size * lax.axis_size("fsdp") * 2
        pieces.append(lax.dynamic_slice_in_dim(small[at : at + total], shard * size, size, 0))
        at += total
    return (
        output,
        tokens_grad,
        pieces[0],
        g_q,
        g_k,
        g_v,
        pieces[2],
        pieces[3],
        g_o,
        pieces[1],
        g_gate,
        g_up,
        g_down,
    )


def solution(mesh):
    token_rows = P(("rep", "fsdp", "seq"), None)
    vec = P(("fsdp", "seq"))
    mat = P(("fsdp", "seq"), None)
    return jax.shard_map(
        on_device,
        mesh=mesh,
        in_specs=(
            token_rows,
            P(("rep", "fsdp"), None),
            vec,
            mat,
            mat,
            mat,
            vec,
            vec,
            mat,
            vec,
            mat,
            mat,
            mat,
            token_rows,
        ),
        out_specs=(
            token_rows,
            token_rows,
            vec,
            mat,
            mat,
            mat,
            vec,
            vec,
            mat,
            vec,
            mat,
            mat,
            mat,
        ),
        check_vma=False,
    )
```

```python
import functools

import jax
import jax.numpy as jnp
from jax import lax
from jax.experimental import pallas as pl
from jax.experimental.pallas import tpu as pltpu
from jax.sharding import PartitionSpec as P

HQ = 16
KV = 8
HD = 128
EPSILON = 1e-06
ROPE_BASE = 1000000.0
SCALE = HD**-0.5
LOG2E = 1.4426950408889634
BLK = 256
BF = jnp.bfloat16
F32 = jnp.float32


def nn(a, b):
    return lax.dot_general(a, b, (((1,), (0,)), ((), ())), preferred_element_type=F32)


def nt(a, b):
    return lax.dot_general(a, b, (((1,), (1,)), ((), ())), preferred_element_type=F32)


def tn(a, b):
    return lax.dot_general(a, b, (((0,), (0,)), ((), ())), preferred_element_type=F32)


def cost(micros):
    return pl.CostEstimate(flops=int(micros * 1.0e7), transcendentals=0, bytes_accessed=0)


def full_spec(shape):
    return pl.BlockSpec(shape, lambda *_: (0,) * len(shape), pipeline_mode=pl.Buffered(1))


class Weight:
    def __init__(self, pieces, base):
        self.pieces = [p for p, _ in pieces]
        self.starts = [s for _, s in pieces]
        self.base = base
        self.shape = (sum(p.shape[0] for p in self.pieces), self.pieces[0].shape[1])


def tiled(name, body, steps, info, inputs, weights, outputs, micros):
    n_in, n_out = len(inputs), len(outputs)
    pieces = [p for w in weights for p in w.pieces]

    def kernel(info_ref, *refs):
        ins = refs[:n_in]
        parts = refs[n_in : n_in + len(pieces)]
        outs = refs[n_in + len(pieces) : n_in + len(pieces) + n_out]
        rest = refs[n_in + len(pieces) + n_out :]
        held, sems = rest[: len(weights)], rest[len(weights) :]

        if pieces:

            @pl.when(pl.program_id(0) == 0)
            def _():
                copies = []
                at = 0
                for n, w in enumerate(weights):
                    for k, piece in enumerate(w.pieces):
                        first = pl.multiple_of(info_ref[w.base + k], 128)
                        target = held[n].at[pl.ds(first, piece.shape[0]), :]
                        copies.append(pltpu.make_async_copy(parts[at], target, sems[0].at[at]))
                        at += 1
                for copy in copies:
                    copy.start()
                for copy in copies:
                    copy.wait()

        body(info_ref, ins, held, outs)

    scratch = [pltpu.VMEM(w.shape, BF) for w in weights]
    if pieces:
        scratch.append(pltpu.SemaphoreType.DMA((len(pieces),)))
    return pl.pallas_call(
        kernel,
        grid_spec=pltpu.PrefetchScalarGridSpec(
            num_scalar_prefetch=1,
            grid=(steps,),
            in_specs=[pl.BlockSpec(block, index) for _, block, index in inputs]
            + [pl.BlockSpec(memory_space=pl.ANY)] * len(pieces),
            out_specs=[pl.BlockSpec(block, index) for _, block, index in outputs],
            scratch_shapes=scratch,
        ),
        out_shape=[shape for shape, _, _ in outputs],
        cost_estimate=cost(micros),
        name=name,
    )(info, *[a for a, _, _ in inputs], *pieces)


def struct(rows, cols, dtype=BF):
    return jax.ShapeDtypeStruct((rows, cols), dtype)


def at_row(t, i):
    return (t, 0)


def once(t, i):
    return (0, 0)


def block(array, index=at_row):
    return (array, (BLK, array.shape[1]), index)


def const(array):
    return (array, array.shape, once)


def result(rows, cols, dtype=BF, index=at_row):
    return (struct(rows, cols, dtype), (BLK, cols), index)


class Order:
    def __init__(self, rows):
        self.half = rows // BLK

    def own(self, t, i):
        return (t + self.half * i[0], 0)

    def other(self, t, i):
        return (t + self.half * (1 - i[0]), 0)

    def global_(self, t, i):
        return ((t + self.half * i[0]) % (2 * self.half), 0)

    def first(self, t, i):
        return (jnp.minimum(t, self.half - 1), 0)

    def second(self, t, i):
        return (jnp.maximum(t - self.half, 0), 0)

    def later(self, t, i):
        return (t + self.half, 0)


def both(order, a, b):
    return jnp.where(pl.program_id(0) < order.half, a[...], b[...])


def project(order, info, tokens, other, gain, weight, cosine, sine, head_gains):
    rows, width = tokens.shape
    cols = weight.shape[1]

    def body(info_ref, ins, held, outs):
        own_ref, other_ref, gain_ref, cos_ref, sin_ref, hg_ref = ins
        normed_ref, qkv_ref, raw_ref = outs
        x = both(order, own_ref, other_ref).astype(F32)
        scale = lax.rsqrt(jnp.mean(x * x, axis=1, keepdims=True) + EPSILON)
        normed = (x * scale * gain_ref[...]).astype(BF)
        normed_ref[...] = normed
        cos_tab, sin_tab = cos_ref[...], sin_ref[...]
        for g in range(cols // 512):
            acc = nn(normed, held[0][:, g * 512 : (g + 1) * 512])
            for h in range(3):
                t = acc[:, h * HD : (h + 1) * HD]
                head_gain = hg_ref[0:1, :] if h < 2 else hg_ref[1:2, :]
                n = t * lax.rsqrt(jnp.mean(t * t, axis=1, keepdims=True) + EPSILON) * head_gain
                turned = n * cos_tab + pltpu.roll(n, HD // 2, 1) * sin_tab
                qkv_ref[:, g * 512 + h * HD : g * 512 + (h + 1) * HD] = turned.astype(BF)
                raw_ref[:, g * 384 + h * HD : g * 384 + (h + 1) * HD] = t.astype(BF)
            qkv_ref[:, g * 512 + 384 : (g + 1) * 512] = acc[:, 384:].astype(BF)

    place = order.global_
    return tiled(
        "project",
        body,
        2 * order.half,
        info,
        [
            block(tokens, order.first),
            block(other, order.second),
            const(gain),
            block(cosine, place),
            block(sine, place),
            const(head_gains),
        ],
        [weight],
        [
            result(2 * rows, width, BF, place),
            result(2 * rows, cols, BF, place),
            result(2 * rows, cols // 4 * 3, BF, place),
        ],
        17,
    )


def times(name, order, info, inputs, index, weight, transposed, micros):
    rows = inputs[0].shape[0] // 2
    cols = weight.shape[0] if transposed else weight.shape[1]

    def body(info_ref, ins, held, outs):
        outs[0][...] = product(ins, held[0], transposed).astype(BF)

    return tiled(
        name,
        body,
        order.half,
        info,
        [block(a, index) for a in inputs],
        [weight],
        [result(rows, cols)],
        micros,
    )[0]


def product(ins, held, transposed):
    total = None
    at = 0
    for a in ins:
        size = a.shape[1]
        if transposed:
            term = nt(a[...], held[:, at : at + size])
        else:
            term = nn(a[...], held[at : at + size, :])
        total = term if total is None else total + term
        at += size
    return total


def mix_own(order, info, attended, tokens, got, gain, weight):
    rows, width = tokens.shape

    def body(info_ref, ins, held, outs):
        att_ref, tok_ref, got_ref, gain_ref = ins
        middle = (
            tok_ref[...].astype(F32) + nn(att_ref[...], held[0][...]) + got_ref[...].astype(F32)
        )
        outs[0][...] = middle
        scale = lax.rsqrt(jnp.mean(middle * middle, axis=1, keepdims=True) + EPSILON)
        outs[1][...] = (middle * scale * gain_ref[...]).astype(BF)

    return tiled(
        "mix_own",
        body,
        order.half,
        info,
        [block(attended, order.own), block(tokens), block(got), const(gain)],
        [weight],
        [result(rows, width, F32), result(rows, width)],
        6,
    )


def mlp(order, info, m_own, m_other, g_own, g_other, w_gu, w_down):
    rows, width = m_own.shape
    half = w_down.shape[0]
    step = 512

    def body(info_ref, ins, held, outs):
        hid_ref, dgu_ref, m_ref, g_ref = outs
        gu, down = held
        m = both(order, ins[0], ins[1])
        g = both(order, ins[2], ins[3])
        m_ref[...] = m
        g_ref[...] = g
        for n in range(0, half, step):
            gate = nn(m, gu[:, n : n + step])
            up = nn(m, gu[:, half + n : half + n + step])
            dh = nt(g, down[n : n + step, :])
            sig = 1.0 / (1.0 + jnp.exp(-gate))
            act = gate * sig
            hid_ref[:, n : n + step] = (act * up).astype(BF)
            dgu_ref[:, n : n + step] = (dh * up * (sig + act * (1.0 - sig))).astype(BF)
            dgu_ref[:, half + n : half + n + step] = (dh * act).astype(BF)

    return tiled(
        "mlp",
        body,
        2 * order.half,
        info,
        [
            block(m_own, order.first),
            block(m_other, order.second),
            block(g_own, order.first),
            block(g_other, order.second),
        ],
        [w_gu, w_down],
        [
            result(2 * rows, half),
            result(2 * rows, 2 * half),
            result(2 * rows, width),
            result(2 * rows, width),
        ],
        30,
    )


def norm_back(d, v, gain):
    r = lax.rsqrt(jnp.mean(v * v, axis=1, keepdims=True) + EPSILON)
    n = v * r
    scaled = d * gain
    dv = r * (scaled - n * jnp.mean(scaled * n, axis=1, keepdims=True))
    return dv, jnp.sum(d * n, axis=0, keepdims=True)


def add_over_steps(ref, value):
    @pl.when(pl.program_id(0) == 0)
    def _():
        ref[...] = value

    @pl.when(pl.program_id(0) > 0)
    def _():
        ref[...] += value


def branch_own(order, info, d_gu, got, middle, cot, gain, weight):
    rows, width = middle.shape

    def body(info_ref, ins, held, outs):
        d_ref, got_ref, mid_ref, cot_ref, gain_ref = ins
        d = product([d_ref], held[0], True) + got_ref[...].astype(F32)
        dv, dg = norm_back(d, mid_ref[...], gain_ref[...])
        d_middle = cot_ref[...].astype(F32) + dv
        outs[0][...] = d_middle
        outs[1][...] = d_middle.astype(BF)
        add_over_steps(outs[2], dg)

    return tiled(
        "branch_own",
        body,
        order.half,
        info,
        [block(d_gu), block(got), block(middle), block(cot), const(gain)],
        [weight],
        [
            result(rows, width, F32),
            result(rows, width),
            (struct(1, width, F32), (1, width), once),
        ],
        11,
    )


def attended_back(order, info, own, other, weight):
    rows, width = own.shape

    def body(info_ref, ins, held, outs):
        branch = both(order, ins[0], ins[1])
        outs[1][...] = branch
        outs[0][...] = nt(branch, held[0][...]).astype(BF)

    place = order.global_
    return tiled(
        "attended_back",
        body,
        2 * order.half,
        info,
        [block(own, order.first), block(other, order.second)],
        [weight],
        [result(2 * rows, weight.shape[0], BF, place), result(2 * rows, width, BF, place)],
        8,
    )


def tokens_own(order, info, d_parts, got, tokens, d_middle, gain, weight):
    rows, width = tokens.shape

    def body(info_ref, ins, held, outs):
        parts, (got_ref, tok_ref, mid_ref, gain_ref) = ins[: len(d_parts)], ins[len(d_parts) :]
        d = product(parts, held[0], True) + got_ref[...].astype(F32)
        dv, dg = norm_back(d, tok_ref[...].astype(F32), gain_ref[...])
        outs[0][...] = mid_ref[...] + dv
        add_over_steps(outs[1], dg)

    return tiled(
        "tokens_own",
        body,
        order.half,
        info,
        [block(d, order.own) for d in d_parts]
        + [block(got), block(tokens), block(d_middle), const(gain)],
        [weight],
        [result(rows, width, F32), (struct(1, width, F32), (1, width), once)],
        9,
    )


def output_own(order, info, hidden, middle, got, weight):
    rows, width = middle.shape

    def body(info_ref, ins, held, outs):
        hid_ref, mid_ref, got_ref = ins
        total = mid_ref[...] + nn(hid_ref[...], held[0][...]) + got_ref[...].astype(F32)
        outs[0][...] = total.astype(BF)

    return tiled(
        "output_own",
        body,
        order.half,
        info,
        [block(hidden), block(middle), block(got)],
        [weight],
        [result(rows, width)],
        6,
    )[0]


def stack_heads(block):
    return jnp.concatenate([block[:, :HD], block[:, HD:]], axis=0)


def attend_kernel(low_ref, qkv_ref, start_ref, out_ref, lse_ref, acc, total):
    blocks = qkv_ref.shape[0] // BLK

    def query_block(qb, carry):
        r0 = pl.multiple_of(qb * BLK, BLK)
        q2 = stack_heads(qkv_ref[pl.ds(r0, BLK), 0:256])
        first = start_ref[pl.ds(r0, BLK), :]
        first2 = jnp.concatenate([first, first], axis=0)

        def tile(k0, diagonal):
            k = qkv_ref[pl.ds(k0, BLK), 256:384]
            v = qkv_ref[pl.ds(k0, BLK), 384:512]
            s = nt(q2, k) * (SCALE * LOG2E)
            col = lax.broadcasted_iota(jnp.int32, (2 * BLK, BLK), 1)
            mask = col >= first2 - k0
            if diagonal:
                row = lax.broadcasted_iota(jnp.int32, (2 * BLK, BLK), 0) & (BLK - 1)
                mask = mask & (col <= row)
            p = jnp.where(mask, jnp.exp2(s), 0.0)
            part = p[:, :HD]
            for n in range(1, BLK // HD):
                part = part + p[:, n * HD : (n + 1) * HD]
            return part, nn(p.astype(BF), v)

        part, mixed = tile(r0, True)
        total[...] = part
        acc[...] = mixed

        def step(kb, inner):
            more, mixed_more = tile(pl.multiple_of(kb * BLK, BLK), False)
            total[...] += more
            acc[...] += mixed_more
            return inner

        lax.fori_loop(low_ref[qb], qb, step, 0)
        sums = total[...]
        o = (acc[...] / jnp.sum(sums, axis=1, keepdims=True)).astype(BF)
        out_ref[pl.ds(r0, BLK), 0:HD] = o[:BLK]
        out_ref[pl.ds(r0, BLK), HD : 2 * HD] = o[BLK:]
        line = jnp.log2(jnp.sum(jnp.transpose(sums), axis=0, keepdims=True))
        lse_ref[0, 0:1, pl.ds(r0, BLK)] = line[:, :BLK]
        lse_ref[0, 1:2, pl.ds(r0, BLK)] = line[:, BLK:]
        return carry

    lax.fori_loop(0, blocks, query_block, 0)


def attend(low, qkv, start, at, groups, earlier=None):
    length, cols = qkv.shape
    whole = cols // 512
    anywhere = [pl.BlockSpec(memory_space=pl.ANY)] * (2 if earlier else 0)

    def body(low_ref, qkv_ref, start_ref, *rest):
        attend_kernel(low_ref, qkv_ref, start_ref, *rest[len(anywhere) :])

    return pl.pallas_call(
        body,
        grid_spec=pltpu.PrefetchScalarGridSpec(
            num_scalar_prefetch=1,
            grid=(groups,),
            in_specs=[
                pl.BlockSpec((length, 512), lambda g, low: (0, g + at)),
                full_spec((length, 1)),
                *anywhere,
            ],
            out_specs=[
                pl.BlockSpec((length, 256), lambda g, low: (0, g + at)),
                pl.BlockSpec((1, 2, length), lambda g, low: (g + at, 0, 0)),
            ],
            scratch_shapes=[
                pltpu.VMEM((2 * BLK, HD), F32),
                pltpu.VMEM((2 * BLK, HD), F32),
            ],
        ),
        out_shape=[
            jax.ShapeDtypeStruct((length, whole * 256), BF),
            jax.ShapeDtypeStruct((whole, 2, length), F32),
        ],
        input_output_aliases={3: 0, 4: 1} if earlier else {},
        cost_estimate=cost(11.5 * groups),
        name="attend",
    )(low, qkv, start.reshape(length, 1), *(earlier or ()))


def head_back(d, raw, gain, cosine, sine):
    dn = d * cosine + pltpu.roll(d * sine, HD // 2, 1)
    raw = raw.astype(F32)
    r = lax.rsqrt(jnp.mean(raw * raw, axis=1, keepdims=True) + EPSILON)
    n = raw * r
    dg = jnp.sum(dn * n, axis=0, keepdims=True)
    scaled = dn * gain
    dv = r * (scaled - n * jnp.mean(scaled * n, axis=1, keepdims=True))
    return dv.astype(BF), dg


def attend_back_kernel(
    low_ref,
    qkv_ref,
    do_ref,
    o_ref,
    lse_ref,
    start_ref,
    raw_ref,
    cos_ref,
    sin_ref,
    hg_ref,
    out_ref,
    dg_ref,
    dk_acc,
    dv_acc,
    dq_acc,
):
    blocks = qkv_ref.shape[0] // BLK
    dg_ref[...] = jnp.zeros_like(dg_ref)

    def query_block(qb, carry):
        r0 = pl.multiple_of(qb * BLK, BLK)
        rows = pl.ds(r0, BLK)
        q2 = stack_heads(qkv_ref[rows, 0:256])
        do2 = stack_heads(do_ref[rows, :])
        o2 = stack_heads(o_ref[rows, :])
        delta = jnp.sum(jnp.transpose(do2.astype(F32) * o2.astype(F32)), axis=0, keepdims=True)
        lse = jnp.concatenate([lse_ref[0, 0:1, rows], lse_ref[0, 1:2, rows]], axis=1)
        first = start_ref[0:1, rows]
        first2 = jnp.concatenate([first, first], axis=1)

        def tile(k0, diagonal):
            k = qkv_ref[pl.ds(k0, BLK), 256:384]
            v = qkv_ref[pl.ds(k0, BLK), 384:512]
            key = lax.broadcasted_iota(jnp.int32, (BLK, 2 * BLK), 0)
            mask = key >= first2 - k0
            if diagonal:
                query = lax.broadcasted_iota(jnp.int32, (BLK, 2 * BLK), 1) & (BLK - 1)
                mask = mask & (key <= query)
            p = jnp.where(mask, jnp.exp2(nt(k, q2) * (SCALE * LOG2E) - lse), 0.0)
            ds = (p * (nt(v, do2) - delta)).astype(BF)
            return nn(ds, q2), nn(p.astype(BF), do2), tn(ds, k)

        dk, dv, dq = tile(r0, True)
        dk_acc[rows, :] = dk
        dv_acc[rows, :] = dv
        dq_acc[...] = dq

        def step(kb, inner):
            k0 = pl.multiple_of(kb * BLK, BLK)
            dk, dv, dq = tile(k0, False)
            dk_acc[pl.ds(k0, BLK), :] += dk
            dv_acc[pl.ds(k0, BLK), :] += dv
            dq_acc[...] += dq
            return inner

        lax.fori_loop(low_ref[qb], qb, step, 0)
        cosine = cos_ref[rows, :]
        sine = sin_ref[rows, :]
        for h in range(2):
            d_raw, dg = head_back(
                dq_acc[h * BLK : (h + 1) * BLK, :] * SCALE,
                raw_ref[rows, h * HD : (h + 1) * HD],
                hg_ref[0:1, :],
                cosine,
                sine,
            )
            out_ref[rows, h * HD : (h + 1) * HD] = d_raw
            dg_ref[0:1, :] += dg
        return carry

    lax.fori_loop(0, blocks, query_block, 0)

    def key_block(kb, carry):
        rows = pl.ds(pl.multiple_of(kb * BLK, BLK), BLK)
        d_raw, dg = head_back(
            dk_acc[rows, :] * SCALE,
            raw_ref[rows, 256:384],
            hg_ref[1:2, :],
            cos_ref[rows, :],
            sin_ref[rows, :],
        )
        out_ref[rows, 256:384] = d_raw
        out_ref[rows, 384:512] = dv_acc[rows, :].astype(BF)
        dg_ref[1:2, :] += dg
        return carry

    lax.fori_loop(0, blocks, key_block, 0)


def attend_back(low, qkv, d_att, att, lse, start, raw, cosine, sine, head_gains, at, earlier):
    length = qkv.shape[0]
    anywhere = [] if earlier is None else [pl.BlockSpec(memory_space=pl.ANY)]

    def body(*refs):
        attend_back_kernel(*refs[:10], *refs[10 + len(anywhere) :])

    column = lambda n: pl.BlockSpec((length, n), lambda g, low: (0, g + at))
    return pl.pallas_call(
        body,
        grid_spec=pltpu.PrefetchScalarGridSpec(
            num_scalar_prefetch=1,
            grid=(1,),
            in_specs=[
                column(512),
                column(256),
                column(256),
                pl.BlockSpec((1, 2, length), lambda g, low: (g + at, 0, 0)),
                full_spec((1, length)),
                column(384),
                full_spec((length, HD)),
                full_spec((length, HD)),
                full_spec((2, HD)),
                *anywhere,
            ],
            out_specs=[
                pl.BlockSpec((length, 512), lambda g, low: (0, at % 3)),
                pl.BlockSpec((2, HD), lambda g, low: (0, 0)),
            ],
            scratch_shapes=[
                pltpu.VMEM((length, HD), F32),
                pltpu.VMEM((length, HD), F32),
                pltpu.VMEM((2 * BLK, HD), F32),
            ],
        ),
        out_shape=[
            jax.ShapeDtypeStruct((length, 1536 if at < 3 else 512), BF),
            jax.ShapeDtypeStruct((2, HD), F32),
        ],
        input_output_aliases={} if earlier is None else {10: 0},
        cost_estimate=cost(21),
        name="attend_back",
    )(low, qkv, d_att, att, lse, start.reshape(1, length), raw, cosine, sine, head_gains, *([] if earlier is None else [earlier]))


def core_heads(c):
    return (2 * c, 2 * c + 1, 4 + 2 * c, 5 + 2 * c)


def qkv_columns(c):
    out = []
    for kv in core_heads(c):
        out += [(0, kv * 256, 256), (1, kv * HD, HD), (2, kv * HD, HD)]
    return out


def gu_columns(c, quarter):
    return [(n, k * quarter, quarter) for n in range(2) for k in (c, 2 + c)]


def pack(name, info, arrays, layout):
    rows = arrays[0].shape[0]
    cols = sum(a.shape[1] for a in arrays) // 2

    def body(info_ref, ins, held, outs):
        for c in range(2):

            @pl.when(info_ref[0] == c)
            def _():
                for target, half in ((outs[0], c), (outs[1], 1 - c)):
                    at = 0
                    for n, first, size in layout(half):
                        target[:, at : at + size] = ins[n][:, first : first + size]
                        at += size

    return tiled(
        name,
        body,
        1,
        info,
        [const(a) for a in arrays],
        [],
        [(struct(rows, cols), (rows, cols), once)] * 2,
        3,
    )


def unpack(name, info, keeps, gots, widths, layout):
    rows = keeps[0].shape[0]
    count = len(keeps)

    def body(info_ref, ins, held, outs):
        for c in range(2):

            @pl.when(info_ref[0] == c)
            def _():
                for half in range(2):
                    source = ins[:count] if half == c else ins[count:]
                    at = 0
                    for n, first, size in layout(half):
                        ref = source[at // source[0].shape[1]]
                        col = at % source[0].shape[1]
                        outs[n][:, first : first + size] = ref[:, col : col + size].astype(F32)
                        at += size

    return tiled(
        name,
        body,
        1,
        info,
        [const(a) for a in keeps + gots],
        [],
        [(struct(rows, w, F32), (rows, w), once) for w in widths],
        4,
    )


def swap(value, axis, bit=0):
    size = lax.axis_size(axis)
    return lax.ppermute(value, axis, [(i, i ^ (1 << bit)) for i in range(size)])


def ordered(first_is_mine, mine, other):
    return jnp.where(
        first_is_mine,
        jnp.concatenate([mine, other], axis=0),
        jnp.concatenate([other, mine], axis=0),
    )


def part(value, index, count, axis=0):
    size = value.shape[axis] // count
    return lax.dynamic_slice_in_dim(value, index * size, size, axis)


def gather_any(value):
    return lax.all_gather(value, ("fsdp", "seq"), axis=0, tiled=True)


def fence(*values):
    return lax.optimization_barrier(values)


class Sum:
    def __init__(self, grad, row, replica):
        self.row, self.replica = row, replica
        self.value = grad.reshape(2, 2, grad.shape[0] // 4, grad.shape[1])

    def send(self, axis):
        self.at = (0, self.row) if axis == "fsdp" else (1, self.replica % 2)
        dim, mine = self.at
        self.got = swap(part(self.value, 1 - mine, 2, dim), axis)
        return self

    def add(self):
        dim, mine = self.at
        self.value = part(self.value, mine, 2, dim) + self.got
        return self

    def flat(self):
        return self.value.reshape(-1, self.value.shape[-1])

STRIP = 512


def strips(*values):
    return jnp.concatenate(
        [v[:, at : at + STRIP] for v in values for at in range(0, v.shape[1], STRIP)], axis=0
    )


def halve(value, replica, bit):
    return swap(part(value, 1 - ((replica >> bit) & 1), 2), "rep", bit)


def add_half(value, got, replica, bit):
    return part(value, (replica >> bit) & 1, 2) + got


def double(value, got, replica, bit):
    return ordered((replica >> bit) & 1 == 0, value, got)


def finish_gu(info, values, gots, quarter):
    rows = gots[0].shape[0] * STRIP // (2 * quarter)
    piece = 256

    def body(info_ref, ins, held, outs):
        for c in range(2):
            for side in range(2):

                @pl.when((info_ref[0] == c) & (info_ref[1] == side))
                def _():
                    for n in range(len(gots)):
                        own, got = ins[2 * n + (c != side)], ins[2 * len(gots) + n]
                        for half, ref in ((c, own), (1 - c, got)):
                            for at in range(0, 2 * quarter, piece):
                                r, col = at // STRIP * rows, at % STRIP
                                k, to = at // quarter, at % quarter
                                to += (half + 2 * k) * quarter
                                outs[n][:, to : to + piece] = ref[
                                    r : r + rows, col : col + piece
                                ].astype(F32)

    return tiled(
        "finish_gu",
        body,
        1,
        info,
        [const(a) for pair in values for a in pair] + [const(g) for g in gots],
        [],
        [(struct(rows, 4 * quarter, F32), (rows, 4 * quarter), once)] * len(gots),
        5,
    )


def finish_rows(info, values, firsts, width):
    strips_n = width // STRIP
    sizes = [(v[0].shape[0] - first) // strips_n for v, first in zip(values, firsts)]

    def body(info_ref, ins, held, outs):
        for side in range(2):

            @pl.when(info_ref[1] == side)
            def _():
                for n, (first, rows) in enumerate(zip(firsts, sizes)):
                    for which in range(2):
                        to = rows * (side if which == 0 else 1 - side)
                        for k in range(strips_n):
                            outs[n][to : to + rows, k * STRIP : (k + 1) * STRIP] = ins[
                                2 * n + which
                            ][first + k * rows : first + (k + 1) * rows, :].astype(F32)

    return tiled(
        "finish_rows",
        body,
        1,
        info,
        [const(a) for pair in values for a in pair],
        [],
        [(struct(2 * r, width, F32), (2 * r, width), once) for r in sizes],
        5,
    )


def land(sums, other):
    *gots, other = fence(*[s.got for s in sums], other)
    for s, got in zip(sums, gots):
        s.got = got
    return other


def take_rows(full, core):
    quarters = full.reshape(4, full.shape[0] // 4, full.shape[1])
    return jnp.concatenate(
        [
            lax.dynamic_index_in_dim(quarters, core, 0, keepdims=False),
            lax.dynamic_index_in_dim(quarters, 2 + core, 0, keepdims=False),
        ],
        axis=0,
    )


def whole_cols(core, mine, send):
    halves = jnp.where(core == 0, mine, send), jnp.where(core == 0, send, mine)
    full = [gather_any(h) for h in halves]
    return jnp.where(core == 0, full[0], full[1])


def scatter_any(full):
    shard = lax.psum_scatter(full, ("fsdp", "seq"), scatter_dimension=0, tiled=True)
    return lax.psum(shard, "rep")


def any_rows(core, grad):
    quarter = grad.shape[0] // 2
    full = jnp.zeros((4, quarter, grad.shape[1]), BF)
    full = lax.dynamic_update_slice(full, grad[None, :quarter], (core, 0, 0))
    full = lax.dynamic_update_slice(full, grad[None, quarter:], (2 + core, 0, 0))
    return scatter_any(full.reshape(4 * quarter, grad.shape[1]))


def any_cols(core, grads):
    keeps, gots = [], []
    for grad in grads:
        halves = [scatter_any(jnp.where(core == c, grad, jnp.zeros_like(grad))) for c in range(2)]
        keeps.append(jnp.where(core == 0, halves[0], halves[1]))
        gots.append(jnp.where(core == 0, halves[1], halves[0]))
    return keeps, gots


def gather_small(vec):
    value = vec[None, :]
    for axis in ("seq", "fsdp"):
        size = lax.axis_size(axis)
        if size & (size - 1):
            return gather_any(vec[None, :])
        for bit in range(size.bit_length() - 1):
            got = lax.ppermute(value, axis, [(i, i ^ (1 << bit)) for i in range(size)])
            value = ordered((lax.axis_index(axis) >> bit) % 2 == 0, value, got)
    return value


def sum_small(value):
    for axis in ("seq", "fsdp", "rep"):
        size = lax.axis_size(axis)
        if size & (size - 1):
            value = lax.psum(value, axis)
            continue
        for bit in range(size.bit_length() - 1):
            value = value + lax.ppermute(value, axis, [(i, i ^ (1 << bit)) for i in range(size)])
    return value


def on_device(
    tokens,
    segments,
    attn_norm,
    w_q,
    w_k,
    w_v,
    q_norm,
    k_norm,
    w_o,
    mlp_norm,
    w_gate,
    w_up,
    w_down,
    cotangent,
):
    core = lax.axis_index("seq")
    row = lax.axis_index("fsdp")
    replica = lax.axis_index("rep")
    rep_size = lax.axis_size("rep")
    pairs = lax.axis_size("fsdp") == 2 and rep_size == 8
    rows, width = tokens.shape
    length = 2 * rows
    order = Order(rows)
    quarter = w_gate.shape[1] // 4
    gu_layout = functools.partial(gu_columns, quarter=quarter)
    side = replica % 2

    def starts(size, blocks):
        return [size * b for b in blocks]

    if pairs:
        quad = [2 * row + core, 2 * row + 1 - core, 2 * (1 - row) + core, 2 * (1 - row) + 1 - core]
        near, far = 2 * (1 - row) + core, 2 * (1 - row) + 1 - core
        gu_far = [jnp.where(side == 0, near, far), jnp.where(side == 0, far, near)]
        o_rows, d_rows = w_o.shape[0], w_down.shape[0]
        layout = (
            starts(w_q.shape[0], quad[:2] + gu_far)
            + [o_rows * row, o_rows * (1 - row)]
            + starts(w_gate.shape[0], quad[:2] + gu_far)
            + [d_rows * row, d_rows * (1 - row)]
        )
        bases = (2, 6, 8, 12)
    else:
        layout = [0 * core] * 4
        bases = (2, 3, 4, 5)
    info = jnp.stack([core, side] + layout).astype(jnp.int32)

    sizes = (attn_norm.shape[0], mlp_norm.shape[0], q_norm.shape[0], k_norm.shape[0])
    gains = gather_small(jnp.concatenate([attn_norm, mlp_norm, q_norm, k_norm])).astype(F32)
    offsets = [0, sizes[0], sizes[0] + sizes[1], sizes[0] + sizes[1] + sizes[2], sum(sizes)]
    attn_gain, mlp_gain, q_gain, k_gain = (
        gains[:, offsets[n] : offsets[n + 1]].reshape(1, -1) for n in range(4)
    )
    head_gains = jnp.concatenate([q_gain, k_gain], axis=0)

    mine, send = pack("pack_qkv", info, [w_q, w_k, w_v], qkv_columns)
    got = swap(send, "seq")
    tokens_other = swap(tokens, "seq")
    if pairs:
        here = swap(jnp.where(side == 0, mine, got), "fsdp")
        wqkv_near = [mine, got]
        got, w_gate, w_up = fence(got, w_gate, w_up)
        gu_mine, send = pack("pack_gu", info, [w_gate, w_up], gu_layout)
        gu_got = swap(send, "seq")
        gu_here = jnp.where(side == 0, gu_mine, gu_got)
        here, attn_gain, head_gains, gu_here, w_o, segments = fence(
            here, attn_gain, head_gains, gu_here, w_o, segments
        )
        there = swap(here, "rep")
        gu_here, o_there = swap(gu_here, "fsdp"), swap(w_o, "fsdp")
        wqkv = Weight(list(zip([*wqkv_near, here, there], layout[:4])), bases[0])
    else:
        wqkv = Weight([(whole_cols(core, mine, send), 0)], bases[0])
        wo = Weight([(take_rows(gather_any(w_o), core), 0)], bases[1])
        mine, send = pack("pack_gu", info, [w_gate, w_up], gu_layout)
        wgu = Weight([(whole_cols(core, mine, send), 0)], bases[2])
        wd = Weight([(take_rows(gather_any(w_down), core), 0)], bases[3])

    cot_other = swap(cotangent, "seq")

    seg = segments[0]
    start = jnp.sum((seg[None, :] < seg[:, None]).astype(jnp.int32), axis=1)
    position = (jnp.arange(length, dtype=jnp.int32) - start).astype(F32)
    inverse = ROPE_BASE ** (jnp.arange(HD // 2, dtype=F32) * (-2.0 / HD))
    angles = position[:, None] * inverse[None, :]
    cos_half, sin_half = jnp.cos(angles), jnp.sin(angles)
    cosine = jnp.concatenate([cos_half, cos_half], axis=1)
    sine = jnp.concatenate([-sin_half, sin_half], axis=1)
    low = start[::BLK] // BLK

    normed, qkv, raw = project(
        order, info, tokens, tokens_other, attn_gain, wqkv, cosine, sine, head_gains
    )
    done = attend(low, qkv, start, 0, 1)
    if pairs:
        *done, gu_here, o_there, w_down = fence(*done, gu_here, o_there, w_down)
        wo = Weight(list(zip([w_o, o_there], layout[4:6])), bases[1])
        gu_there = swap(gu_here, "rep")
        d_there = swap(w_down, "fsdp")
    done = attend(low, qkv, start, 1, 2, done)
    attended, lse = attend(low, qkv, start, 3, 1, done)

    sent = times("mix_other", order, info, [attended], order.other, wo, False, 5)
    if pairs:
        sent, gu_there, d_there = fence(sent, gu_there, d_there)
        wgu = Weight(list(zip([gu_mine, gu_got, gu_here, gu_there], layout[6:10])), bases[2])
        wd = Weight(list(zip([w_down, d_there], layout[10:])), bases[3])
    middle, m_own = mix_own(order, info, attended, tokens, swap(sent, "seq"), mlp_gain, wo)
    hidden, d_gu, m_all, g_all = mlp(
        order, info, m_own, swap(m_own, "seq"), cotangent, cot_other, wgu, wd
    )
    g_down = tn(hidden, g_all).astype(BF)
    if pairs:
        d_gu, g_down = fence(d_gu, g_down)

    sent = times("branch_other", order, info, [d_gu], order.later, wgu, True, 9)
    got = swap(sent, "seq")
    m_all, sent = fence(m_all, sent)
    g_gu = tn(m_all, d_gu).astype(BF)
    d_gu, got, g_gu = fence(d_gu, got, g_gu)
    d_middle, d_branch, dg_mlp = branch_own(
        order, info, d_gu, got, middle, cotangent, mlp_gain, wgu
    )
    branch_other = swap(d_branch, "seq")
    d_att, branch_all = attended_back(order, info, d_branch, branch_other, wo)
    g_o = tn(attended, branch_all).astype(BF)
    if pairs:
        down = Sum(g_down, row, replica).send("rep")
        gate, up = (
            Sum(g_gu[:, n * 2 * quarter : (n + 1) * 2 * quarter], row, replica).send("fsdp")
            for n in range(2)
        )
        o_sum = Sum(g_o, row, replica).send("fsdp")
        d_att, g_o = fence(d_att, g_o)

    def back(at, earlier=None):
        return attend_back(
            low, qkv, d_att, attended, lse, start, raw, cosine, sine, head_gains, at, earlier
        )

    d_qkv0, dg0 = back(0)
    if pairs:
        d_qkv0 = land([down, gate], d_qkv0)
        down.add().send("fsdp")
        gate.add().send("rep")
    d_qkv0, dg1 = back(1, d_qkv0)
    if pairs:
        d_qkv0 = land([down, gate, up], d_qkv0)
        early = strips(gate.add().flat(), down.add().flat())
        early_got = halve(early, replica, 1)
        up.add().send("rep")
    d_qkv0, dg2 = back(2, d_qkv0)
    if pairs:
        early_got, up.got, o_sum.got, d_qkv0 = fence(early_got, up.got, o_sum.got, d_qkv0)
        early = add_half(early, early_got, replica, 1)
        early_got = halve(early, replica, 2)
        o_sum.add().send("rep")
    g_qkv0 = tn(normed, d_qkv0).astype(BF)
    if pairs:
        qkv0 = Sum(g_qkv0, row, replica).send("fsdp")
    d_att, g_qkv0 = fence(d_att, g_qkv0)
    d_qkv1, dg3 = back(3)
    if pairs:
        early_got, o_sum.got, qkv0.got, d_qkv1 = fence(early_got, o_sum.got, qkv0.got, d_qkv1)
    g_qkv1 = tn(normed, d_qkv1).astype(BF)
    d_qkv1, g_qkv1 = fence(d_qkv1, g_qkv1)
    if pairs:
        qkv1 = Sum(g_qkv1, row, replica).send("fsdp")
        early = add_half(early, early_got, replica, 2)
        early_got = swap(early, "rep", 2)
        late = strips(up.add().flat(), o_sum.add().flat())
        late_got = halve(late, replica, 1)
        qkv0.add().send("rep")

    sent = times("tokens_other", order, info, [d_qkv0, d_qkv1], order.other, wqkv, True, 6)
    if pairs:
        early_got, late_got, qkv0.got, qkv1.got, sent = fence(
            early_got, late_got, qkv0.got, qkv1.got, sent
        )
        qkv1.add().send("rep")
        early = double(early, early_got, replica, 2)
        early_got = swap(early, "rep", 1)
        late = add_half(late, late_got, replica, 1)
        late_got = halve(late, replica, 2)
    hidden, sent = fence(hidden, sent)
    out_sent = times("output_other", order, info, [hidden], order.later, wd, False, 6)
    if pairs:
        early_got, late_got, qkv1.got, out_sent = fence(early_got, late_got, qkv1.got, out_sent)
        last = jnp.concatenate([qkv0.add().flat(), qkv1.add().flat()], axis=1)
        last_got = halve(last, replica, 1)
        early = double(early, early_got, replica, 1)
        early_far = swap(early, "rep", 0)
        late = add_half(late, late_got, replica, 2)
        late_got = swap(late, "rep", 2)
    sent, out_sent = fence(sent, out_sent)
    got, out_got = swap(sent, "seq"), swap(out_sent, "seq")
    tokens_grad, dg_attn = tokens_own(
        order, info, [d_qkv0, d_qkv1], got, tokens, d_middle, attn_gain, wqkv
    )
    dg_heads = dg0 + dg1 + dg2 + dg3
    small = jnp.concatenate([dg_attn[0], dg_mlp[0], dg_heads[0], dg_heads[1]])
    if pairs:
        late_got, last_got, tokens_grad = fence(late_got, last_got, tokens_grad)
        last = add_half(last, last_got, replica, 1)
        last_got = halve(last, replica, 2)
        late = double(late, late_got, replica, 2)
        late_got = swap(late, "rep", 1)
        hop = swap(small, "seq")
    hidden, tokens_grad = fence(hidden, tokens_grad)
    output = output_own(order, info, hidden, middle, out_got, wd)
    if pairs:
        last_got, hop, output = fence(last_got, hop, output)
        last = add_half(last, last_got, replica, 2)
        last_got = swap(last, "rep", 2)
        small = small + hop
        hop = swap(small, "fsdp")
        home = core == side
        gu_rows = early.shape[0] // 2

        def finish(own, far):
            send = jnp.where(home, far[:gu_rows], own[:gu_rows])
            columns = finish_gu(info, [(own, far)], [swap(send, "seq")], quarter)
            return columns + finish_rows(info, [(own, far)], [gu_rows], width)

        late_got, early_far, output = fence(late_got, early_far, output)
        late = double(late, late_got, replica, 1)
        late_far = swap(late, "rep", 0)
        g_gate, g_down = finish(early, early_far)

        last_got, hop, g_gate, g_down = fence(last_got, hop, g_gate, g_down)
        last = double(last, last_got, replica, 2)
        last_got = swap(last, "rep", 1)
        small = small + hop
        hop = swap(small, "rep", 1)

        last_got, hop = fence(last_got, hop)
        last = double(last, last_got, replica, 1)
        last_far = swap(last, "rep", 0)
        small = small + hop
        hop = swap(small, "rep", 2)

        late_far, hop = fence(late_far, hop)
        small = small + hop
        hop = swap(small, "rep", 0)
        g_up, g_o = finish(late, late_far)

        last_far, g_up, g_o, hop = fence(last_far, g_up, g_o, hop)
        small = small + hop
        keep, send = jnp.where(home, last, last_far), jnp.where(home, last_far, last)
        qkv_parts = [keep], [swap(send, "seq")]
    else:
        small = sum_small(small)
        g_down, g_o = (any_rows(core, g).astype(F32) for g in (g_down, g_o))
        qkv_parts = any_cols(core, [jnp.concatenate([g_qkv0, g_qkv1], axis=1)])
        gu_parts = any_cols(core, [g_gu[:, : 2 * quarter], g_gu[:, 2 * quarter :]])
        g_gate, g_up = unpack("unpack_gu", info, *gu_parts, [w_gate.shape[1]] * 2, gu_layout)
    g_q, g_k, g_v = unpack(
        "unpack_qkv", info, *qkv_parts, [a.shape[1] for a in (w_q, w_k, w_v)], qkv_columns
    )

    shard = row * 2 + core
    pieces = []
    at = 0
    for size in sizes:
        total = size * lax.axis_size("fsdp") * 2
        pieces.append(lax.dynamic_slice_in_dim(small[at : at + total], shard * size, size, 0))
        at += total
    return (
        output,
        tokens_grad,
        pieces[0],
        g_q,
        g_k,
        g_v,
        pieces[2],
        pieces[3],
        g_o,
        pieces[1],
        g_gate,
        g_up,
        g_down,
    )


def solution(mesh):
    token_rows = P(("rep", "fsdp", "seq"), None)
    vec = P(("fsdp", "seq"))
    mat = P(("fsdp", "seq"), None)
    return jax.shard_map(
        on_device,
        mesh=mesh,
        in_specs=(
            token_rows,
            P(("rep", "fsdp"), None),
            vec,
            mat,
            mat,
            mat,
            vec,
            vec,
            mat,
            vec,
            mat,
            mat,
            mat,
            token_rows,
        ),
        out_specs=(
            token_rows,
            token_rows,
            vec,
            mat,
            mat,
            mat,
            vec,
            vec,
            mat,
            vec,
            mat,
            mat,
            mat,
        ),
        check_vma=False,
    )
```
